32 devices in a mesh: rep: 1 (over z), kv2: 4 (over y), kv: 8 (over x, core).
Axes of the slice: x: 4, y: 4, z: 1, core: 2. Of those that a mesh axis runs over, the one named last changes fastest.
The devices are a block of a 4x4x8 slice.
Arguments:
- x_embed: bfloat16 [2, 768, 2048], P(None, ('rep', 'kv2', 'kv'))
- w_query: bfloat16 [2, 2048, 2048], replicated
- w_key: bfloat16 [2, 2048, 256], replicated
- w_value: bfloat16 [2, 2048, 256], replicated
- w_out: bfloat16 [2, 2048, 2048], replicated
- w_up: bfloat16 [2, 2048, 11008], replicated
- w_down: bfloat16 [2, 11008, 2048], replicated
- k_pool: bfloat16 [3584, 2, 64, 2, 128], P(('rep', 'kv2', 'kv'))
- v_pool: bfloat16 [3584, 2, 64, 2, 128], P(('rep', 'kv2', 'kv'))
- old_table: int32 [768, 2], P(('rep', 'kv2', 'kv'))
- seq_len: int32 [768], P(('rep', 'kv2', 'kv'))
- src_slot: int32 [512], P(('rep', 'kv2', 'kv'))
- dst_slot: int32 [512], P(('rep', 'kv2', 'kv'))
Outputs:
- output 1: bfloat16 [2, 768, 2048], P(None, ('rep', 'kv2', 'kv'))
- output 2: bfloat16 [3584, 2, 64, 2, 128], P(('rep', 'kv2', 'kv'))
- output 3: bfloat16 [3584, 2, 64, 2, 128], P(('rep', 'kv2', 'kv'))
All inputs are finite; a program needn't handle non-finite values.
Results may differ from the reference program's by a relative error of at most 0.0125823.
Values are sent between devices in bfloat16 or wider.
A program may use at most 768 MiB of HBM per device.

```python
import jax
import jax.numpy as jnp
from jax import lax

MESH_ROWS = 4
MESH_COLS = 8
SEQ_DEV = 24
PAGES = 2
MIG_DEV = 16
D = 2048
HEADS = 16
KV_HEADS = 2
HEAD = 128
FF = 11008
PAGE = 64
LAYERS = 2
DEVICES_PART = MESH_ROWS * MESH_COLS
ROW_SEQS = MESH_COLS * SEQ_DEV
BATCH = DEVICES_PART * SEQ_DEV
SLOTS = 2 * SEQ_DEV * PAGES + MIG_DEV
MOVES = DEVICES_PART * MIG_DEV
ALL_SLOTS = DEVICES_PART * SLOTS


def draw_layout(key):
    keys_list = jax.random.split(key, 7)
    n_pages = jax.random.randint(keys_list[0], (BATCH,), 2, PAGES + 1).at[0].set(PAGES)
    fill_len = jax.random.randint(keys_list[1], (BATCH,), 0, PAGE - 1).at[0].set(PAGE - 2)
    seq_len = (n_pages - 1) * PAGE + fill_len
    dev_ids = jnp.arange(DEVICES_PART, dtype=jnp.int32)
    local_ids = jnp.arange(SLOTS, dtype=jnp.int32)
    slot_caps = jnp.where(dev_ids % MESH_COLS % 2 == 0, SLOTS - MIG_DEV, (SLOTS - MIG_DEV) // 4)
    move_ids = jnp.arange(MOVES, dtype=jnp.int32)
    src_dev = move_ids // MIG_DEV
    target = 2 * (jax.random.permutation(keys_list[2], MOVES) // (2 * MIG_DEV))
    target = jnp.where(target == src_dev, (target + 2) % DEVICES_PART, target)
    order_t = jnp.argsort(target * MOVES + move_ids)
    group_start = jnp.searchsorted(target[order_t], target)
    rank_in = jnp.argsort(order_t) - group_start
    outside = (local_ids[None, :] >= slot_caps[:, None]).astype(jnp.int32)
    prio_dst = jax.random.permutation(keys_list[3], ALL_SLOTS).reshape(DEVICES_PART, SLOTS) + outside * ALL_SLOTS
    dst_slot = target * SLOTS + jnp.argsort(prio_dst, axis=1)[target, rank_in]
    prio_src = jax.random.permutation(keys_list[4], ALL_SLOTS).reshape(DEVICES_PART, SLOTS) + (1 - outside) * ALL_SLOTS
    src_slot = (dev_ids[:, None] * SLOTS + jnp.argsort(prio_src, axis=1)[:, :MIG_DEV]).reshape(MOVES)
    marked = jnp.zeros((ALL_SLOTS,), jnp.int32).at[dst_slot].set(1).reshape(MESH_ROWS, MESH_COLS * SLOTS)
    inside = (1 - outside).reshape(MESH_ROWS, MESH_COLS * SLOTS)
    prio_new = jax.random.permutation(keys_list[5], ALL_SLOTS).reshape(MESH_ROWS, MESH_COLS * SLOTS) + jnp.where(marked == 1, 0, jnp.where(inside == 1, ALL_SLOTS, 2 * ALL_SLOTS))
    slot_order = jnp.argsort(prio_new, axis=1)
    pages_row = n_pages.reshape(MESH_ROWS, ROW_SEQS, 1)
    page_ids = jnp.arange(PAGES, dtype=jnp.int32)[None, None, :]
    is_valid = (page_ids < pages_row).reshape(MESH_ROWS, ROW_SEQS * PAGES)
    is_last = (page_ids == pages_row - 1).reshape(MESH_ROWS, ROW_SEQS * PAGES)
    n_cells = BATCH * PAGES
    cell_key = jax.random.permutation(keys_list[6], n_cells).reshape(MESH_ROWS, ROW_SEQS * PAGES) + jnp.where(is_last, 0, jnp.where(is_valid, n_cells, 2 * n_cells))
    cell_rank = jnp.argsort(jnp.argsort(cell_key, axis=1), axis=1)
    row_base = jnp.arange(MESH_ROWS, dtype=jnp.int32)[:, None] * (MESH_COLS * SLOTS)
    new_slot = jnp.take_along_axis(slot_order, cell_rank, axis=1) + row_base
    new_table = jnp.where(is_valid, new_slot, -1).reshape(BATCH, PAGES)
    slot_move = jnp.full((ALL_SLOTS,), -1, jnp.int32).at[dst_slot].set(move_ids)
    move_idx = slot_move[jnp.maximum(new_table, 0)]
    old_table = jnp.where((new_table >= 0) & (move_idx >= 0), src_slot[jnp.maximum(move_idx, 0)], new_table)
    return old_table.astype(jnp.int32), seq_len.astype(jnp.int32), src_slot.astype(jnp.int32), dst_slot.astype(jnp.int32)


def weight_draw(key, shape):
    return (jax.random.normal(key, shape, jnp.float32) * shape[1] ** -0.5).astype(jnp.bfloat16)


def setup_inputs(seed: int = 0, part: int = 0) -> dict:
    root = jax.random.key(seed)
    shared = jax.random.split(root, 6)
    own = jax.random.split(jax.random.fold_in(root, part), 4)
    pool_shape = (ALL_SLOTS, LAYERS, PAGE, KV_HEADS, HEAD)
    old_table, seq_len, src_slot, dst_slot = draw_layout(own[3])
    return dict(
        x_embed=jax.random.normal(own[0], (2, BATCH, D), jnp.float32).astype(jnp.bfloat16),
        w_query=weight_draw(shared[0], (LAYERS, D, HEADS * HEAD)),
        w_key=weight_draw(shared[1], (LAYERS, D, KV_HEADS * HEAD)),
        w_value=weight_draw(shared[2], (LAYERS, D, KV_HEADS * HEAD)),
        w_out=weight_draw(shared[3], (LAYERS, HEADS * HEAD, D)),
        w_up=weight_draw(shared[4], (LAYERS, D, FF)),
        w_down=weight_draw(shared[5], (LAYERS, FF, D)),
        k_pool=jax.random.normal(own[1], pool_shape, jnp.float32).astype(jnp.bfloat16),
        v_pool=jax.random.normal(own[2], pool_shape, jnp.float32).astype(jnp.bfloat16),
        old_table=old_table,
        seq_len=seq_len,
        src_slot=src_slot,
        dst_slot=dst_slot,
    )


def reference(x_embed, w_query, w_key, w_value, w_out, w_up, w_down, k_pool, v_pool, old_table, seq_len, src_slot, dst_slot):
    move_ids = jnp.arange(MOVES, dtype=jnp.int32)
    slot_move = jnp.full((ALL_SLOTS,), -1, jnp.int32).at[src_slot].set(move_ids)
    move_idx = slot_move[jnp.maximum(old_table, 0)]
    new_table = jnp.where((old_table >= 0) & (move_idx >= 0), dst_slot[jnp.maximum(move_idx, 0)], old_table)
    k_pool = k_pool.at[dst_slot].set(k_pool[src_slot])
    v_pool = v_pool.at[dst_slot].set(v_pool[src_slot])
    seq_ids = jnp.arange(BATCH)
    tok_pos = jnp.arange(PAGES * PAGE)
    q_group = HEADS // KV_HEADS
    step_outs = []
    for step_idx in range(2):
        cur_pos = seq_len + step_idx
        w_slot = new_table[seq_ids, cur_pos // PAGE]
        w_off = cur_pos % PAGE

        def layer_body(layer_state, layer_in):
            hidden, k_cache, v_cache = layer_state
            layer_idx, wq_l, wk_l, wv_l, wo_l, up_l, down_l = layer_in
            query = jnp.dot(hidden, wq_l, preferred_element_type=jnp.float32).astype(jnp.bfloat16)
            k_new = jnp.dot(hidden, wk_l, preferred_element_type=jnp.float32).astype(jnp.bfloat16).reshape(BATCH, KV_HEADS, HEAD)
            v_new = jnp.dot(hidden, wv_l, preferred_element_type=jnp.float32).astype(jnp.bfloat16).reshape(BATCH, KV_HEADS, HEAD)
            k_cache = k_cache.at[w_slot, layer_idx, w_off].set(k_new)
            v_cache = v_cache.at[w_slot, layer_idx, w_off].set(v_new)

            def attend(seq_in):
                q_row, table_row, limit_pos = seq_in
                page_sel = jnp.maximum(table_row, 0)
                page_keys = k_cache[page_sel, layer_idx].reshape(PAGES * PAGE, KV_HEADS, HEAD).astype(jnp.float32)
                page_vals = v_cache[page_sel, layer_idx].reshape(PAGES * PAGE, KV_HEADS, HEAD).astype(jnp.float32)
                q_heads = q_row.reshape(KV_HEADS, q_group, HEAD).astype(jnp.float32)
                scores = jnp.einsum('grd,tgd->grt', q_heads, page_keys) * HEAD ** -0.5
                scores = jnp.where(tok_pos <= limit_pos, scores, -1e30)
                attn_w = jax.nn.softmax(scores, axis=-1)
                return jnp.einsum('grt,tgd->grd', attn_w, page_vals).reshape(HEADS * HEAD).astype(jnp.bfloat16)

            attn_out = lax.map(attend, (query, new_table, cur_pos))
            hidden = (hidden.astype(jnp.float32) + jnp.dot(attn_out, wo_l, preferred_element_type=jnp.float32)).astype(jnp.bfloat16)
            up_act = jax.nn.gelu(jnp.dot(hidden, up_l, preferred_element_type=jnp.float32)).astype(jnp.bfloat16)
            hidden = (hidden.astype(jnp.float32) + jnp.dot(up_act, down_l, preferred_element_type=jnp.float32)).astype(jnp.bfloat16)
            return (hidden, k_cache, v_cache), None

        layer_xs = (jnp.arange(LAYERS), w_query, w_key, w_value, w_out, w_up, w_down)
        (hidden, k_pool, v_pool), _ = lax.scan(layer_body, (x_embed[step_idx], k_pool, v_pool), layer_xs)
        step_outs.append(hidden)
    return jnp.stack(step_outs), k_pool, v_pool
```

```python
import functools

import jax
import jax.numpy as jnp
from jax import lax
from jax.experimental import pallas as pl
from jax.experimental.pallas import tpu as pltpu
from jax.sharding import PartitionSpec as P

MESH = pl.DeviceIdType.MESH
ANY = pl.BlockSpec(memory_space=pl.ANY)
SMEM = pl.BlockSpec(memory_space=pltpu.SMEM)
VMEM = pl.BlockSpec(memory_space=pltpu.VMEM)
F32 = jnp.float32
BF16 = jnp.bfloat16
NEG = -1e30


def flat_id(n_cols):
    return lax.axis_index('kv2') * n_cols + lax.axis_index('kv')


def where_is(flat, n_cols):
    return {'kv2': flat // n_cols, 'kv': flat % n_cols}


def greet_all(n_dev, n_cols):
    me = flat_id(n_cols)
    barrier = pltpu.get_barrier_semaphore()

    @pl.loop(1, n_dev)
    def _(r):
        pl.semaphore_signal(barrier, inc=1, device_id=where_is((me + r) % n_dev, n_cols), device_id_type=MESH)

    pl.semaphore_wait(barrier, n_dev - 1)


def gather_all_kernel(n_dev, n_cols, x_ref, o_ref, local_sem, send_sem, recv_sem):
    me = flat_id(n_cols)
    greet_all(n_dev, n_cols)

    def copy(r, dst, slot):
        return pltpu.make_async_remote_copy(
            src_ref=x_ref, dst_ref=o_ref.at[slot], send_sem=send_sem.at[r], recv_sem=recv_sem.at[r],
            device_id=where_is(dst, n_cols), device_id_type=MESH)

    @pl.loop(1, n_dev)
    def _(r):
        copy(r, (me + r) % n_dev, me).start()

    own = pltpu.make_async_copy(x_ref, o_ref.at[me], local_sem)
    own.start()
    own.wait()

    @pl.loop(1, n_dev)
    def _(r):
        c = copy(r, (me + r) % n_dev, (me + n_dev - r) % n_dev)
        c.wait_send()
        c.wait_recv()


def row_gather_kernel(n_cols, x_ref, o_ref, local_sem, send_sem, recv_sem, fsend_sem, frecv_sem):
    n_chips = n_cols // 2
    kv = lax.axis_index('kv')
    chip, core = kv // 2, kv % 2
    mate = chip * 2 + 1 - core
    barrier = pltpu.get_barrier_semaphore()
    for r in range(1, n_chips):
        pl.semaphore_signal(barrier, inc=1, device_id={'kv': (chip + r) % n_chips * 2 + core}, device_id_type=MESH)
    pl.semaphore_signal(barrier, inc=1, device_id={'kv': mate}, device_id_type=MESH)
    pl.semaphore_wait(barrier, n_chips)

    def copy(r, dst, slot):
        return pltpu.make_async_remote_copy(
            src_ref=x_ref, dst_ref=o_ref.at[slot], send_sem=send_sem.at[r], recv_sem=recv_sem.at[r],
            device_id={'kv': dst}, device_id_type=MESH)

    def forward(r, slot):
        return pltpu.make_async_remote_copy(
            src_ref=o_ref.at[slot], dst_ref=o_ref.at[slot], send_sem=fsend_sem.at[r], recv_sem=frecv_sem.at[r],
            device_id={'kv': mate}, device_id_type=MESH)

    for r in range(1, n_chips):
        copy(r, (chip + r) % n_chips * 2 + core, kv).start()
    copy(0, mate, kv).start()
    own = pltpu.make_async_copy(x_ref, o_ref.at[kv], local_sem)
    own.start()
    own.wait()
    for r in range(1, n_chips):
        slot = (chip + n_chips - r) % n_chips * 2 + core
        copy(r, mate, slot).wait_recv()
        forward(r, slot).start()
    for r in range(1, n_chips):
        copy(r, mate, kv).wait_send()
        forward(r, (chip + n_chips - r) % n_chips * 2 + core).wait_send()
        forward(r, (chip + n_chips - r) % n_chips * 2 + 1 - core).wait_recv()
    c = copy(0, mate, mate)
    c.wait_send()
    c.wait_recv()


def row_exchange_kernel(n_cols, x_ref, y_ref, ox_ref, oy_ref, local_sem, send_sem, recv_sem):
    kv = lax.axis_index('kv')
    barrier = pltpu.get_barrier_semaphore()
    for r in range(1, n_cols):
        pl.semaphore_signal(barrier, inc=1, device_id={'kv': (kv + r) % n_cols}, device_id_type=MESH)
    pl.semaphore_wait(barrier, n_cols - 1)

    def copy(a, r, dst, slot):
        src_ref, dst_ref = ((x_ref, ox_ref), (y_ref, oy_ref))[a]
        return pltpu.make_async_remote_copy(
            src_ref=src_ref.at[dst], dst_ref=dst_ref.at[slot], send_sem=send_sem.at[a, r], recv_sem=recv_sem.at[a, r],
            device_id={'kv': dst}, device_id_type=MESH)

    for r in range(1, n_cols):
        for a in range(2):
            copy(a, r, (kv + r) % n_cols, kv).start()
    own = [pltpu.make_async_copy(s.at[kv], d.at[kv], local_sem.at[a]) for a, (s, d) in enumerate(((x_ref, ox_ref), (y_ref, oy_ref)))]
    for c in own:
        c.start()
    for c in own:
        c.wait()
    for r in range(1, n_cols):
        for a in range(2):
            c = copy(a, r, (kv + r) % n_cols, (kv + n_cols - r) % n_cols)
            c.wait_send()
            c.wait_recv()


def plan_kernel(dims, who_ref, tab_ref, none_ref, pages_ref, info_ref, most_ref, moved, count, seen, sem):
    n_dev, n_cols, n_slots, seq_dev, n_moves, cap, page, magic, shift = dims
    n_chips = n_dev // 2
    o_len, o_src, o_dst = 2 * seq_dev, 3 * seq_dev, 3 * seq_dev + n_moves
    me = who_ref[0]
    row0 = who_ref[1]
    base = me * n_slots
    fill = pltpu.make_async_copy(none_ref, moved, sem)
    fill.start()

    @pl.loop(0, n_chips)
    def _(i):
        count[i] = 0

    @pl.loop(0, n_cols * seq_dev)
    def _(i):
        seen[i] = 0

    @pl.loop(0, n_slots)
    def _(i):
        for f in range(4):
            info_ref[f * n_slots + i] = -1

    @pl.loop(0, n_dev * cap)
    def _(i):
        pages_ref[i] = 0

    fill.wait()

    @pl.loop(0, n_dev)
    def _(d):
        for j in range(n_moves):
            src = tab_ref[d, o_src + j]
            dst = tab_ref[d, o_dst + j]
            m = d * n_moves + j
            moved[src] = dst
            dd = (dst * magic) >> shift
            chip = dd >> 1
            n = count[chip]
            count[chip] = n + 1

            @pl.when(n < 2 * cap)
            def _():
                pages_ref[chip * 2 * cap + n] = m

            @pl.when(dd == me)
            def _():
                info_ref[dst - base] = n
                info_ref[n_slots + dst - base] = m

    def biggest(i, best):
        return jnp.maximum(best, count[i])

    most_ref[0] = lax.fori_loop(0, n_chips, biggest, jnp.int32(0))

    @pl.loop(0, n_cols)
    def _(h):
        @pl.loop(0, seq_dev)
        def _(i):
            b = h * seq_dev + i
            length = tab_ref[row0 + h, o_len + i]
            for j in range(2):
                e = tab_ref[row0 + h, 2 * i + j]
                e0 = jnp.maximum(e, 0)
                mv = moved[e0]
                s = jnp.where(mv >= 0, mv, e0) - base

                @pl.when((e >= 0) & (s >= 0) & (s < n_slots))
                def _():
                    info_ref[2 * n_slots + s] = b
                    info_ref[4 * n_slots + s] = length - page * j

    @pl.loop(0, n_slots)
    def _(s):
        b = info_ref[2 * n_slots + s]

        @pl.when(b >= 0)
        def _():
            info_ref[5 * n_slots + s] = seen[b]
            seen[b] = 1


def pack_kernel(n_moves, src_ref, k_ref, v_ref, *rest):
    *outs, sem = rest

    def copies(m):
        s = src_ref[m]
        for layer, o_ref in enumerate(outs):
            half = o_ref.shape[0] // 2
            for a, pool in enumerate((k_ref, v_ref)):
                yield pltpu.make_async_copy(pool.at[s, layer], o_ref.at[pl.ds(a * half, half), m], sem.at[layer, a, m])

    for m in range(n_moves):
        for c in copies(m):
            c.start()
    for m in range(n_moves):
        for c in copies(m):
            c.wait()


def regroup_kernel(cap, pages_ref, x_ref, o_ref):
    @pl.loop(0, o_ref.shape[0])
    def _(d):
        for n in range(cap):
            o_ref[d, n] = x_ref[pages_ref[d * cap + n]]


def attend_kernel(dims, info_ref, most_ref, who_ref, q_ref, k_ref, v_ref, own_ref, mate_ref, slow_ref, *rest):
    layer, n_slots, blk, group, cap, scale, first = dims
    ko_ref, vo_ref, o_ref, ml_ref, kbuf, vbuf, sem = rest if first else rest[2:]
    g = pl.program_id(0)
    steps = pl.num_programs(0)
    n_key, lanes = k_ref.shape[1:]
    rows = o_ref.shape[1]
    n_ch = kbuf.shape[2]
    over = most_ref[0] > 2 * cap
    core = who_ref[2]

    def fetches(step, i, src_of):
        return [pltpu.make_async_copy(src_of(pl.ds(a * n_ch, n_ch)), buf.at[step % 2, i], sem.at[a, step % 2, i])
                for a, buf in enumerate((kbuf, vbuf))]

    def start(step):
        @pl.loop(0, blk)
        def _(i):
            s = step * blk + i
            n = info_ref[s]
            has = n >= 0
            half = jnp.where(n >= cap, 1, 0)
            pos = n - half * cap

            def go(cond, src_of):
                @pl.when(has & cond)
                def _():
                    for c in fetches(step, i, src_of):
                        c.start()

            go(over, lambda part: slow_ref.at[layer, s, part])
            go(jnp.logical_not(over) & (half == core), lambda part: own_ref.at[part, pos])
            go(jnp.logical_not(over) & (half != core), lambda part: mate_ref.at[part, pos])

    @pl.when(g == 0)
    def _():
        o_ref[...] = jnp.zeros_like(o_ref)
        lane = lax.broadcasted_iota(jnp.int32, ml_ref.shape, 1)
        ml_ref[...] = jnp.where(lane < rows, NEG, 0.0)
        start(0)

    @pl.when(g + 1 < steps)
    def _():
        start(g + 1)

    tile = 16
    tile_row = lax.broadcasted_iota(jnp.int32, (tile, lanes), 0)
    lane = lax.broadcasted_iota(jnp.int32, (rows, n_key), 1)
    row = lax.broadcasted_iota(jnp.int32, (rows, n_key), 0)
    own_head = (lane & 1) == ((row >> 3) & 1)
    late = (lane >> 1) - (row >> 4)
    out_lane = lax.broadcasted_iota(jnp.int32, (rows, lanes), 1)
    out_row = lax.broadcasted_iota(jnp.int32, (rows, lanes), 0)

    @pl.loop(0, blk // group)
    def _(u):
        facts = []
        for t in range(group):
            i = u * group + t
            s = g * blk + i
            has = info_ref[s] >= 0
            b = info_ref[2 * n_slots + s]
            lim = info_ref[4 * n_slots + s]
            used = b >= 0
            b0 = jnp.maximum(b, 0)

            @pl.when(has)
            def _():
                for c in fetches(g, i, lambda part: own_ref.at[part, 0]):
                    c.wait()
                ko_ref[i] = kbuf[g % 2, i].reshape(n_key, lanes)
                vo_ref[i] = vbuf[g % 2, i].reshape(n_key, lanes)

            @pl.when(jnp.logical_not(has))
            def _():
                ko_ref[i] = k_ref[i]
                vo_ref[i] = v_ref[i]

            @pl.when(used & (lim < n_key // 2))
            def _():
                fresh = q_ref[b0, rows:].astype(F32)
                row0 = 2 * lim
                for c in (row0 // tile, jnp.minimum((row0 + 3) // tile, n_key // tile - 1)):
                    at = tile_row + c * tile - row0
                    part = pl.ds(pl.multiple_of(c * tile, tile), tile)
                    for a, ref in enumerate((ko_ref, vo_ref)):
                        x = ref[i, part].astype(F32)
                        for r in range(4):
                            x = jnp.where(at == r, fresh[4 * a + r:4 * a + r + 1], x)
                        ref[i, part] = x.astype(BF16)

            facts.append((i, used, b0, lim, info_ref[5 * n_slots + s]))
        done = []
        for i, used, b0, lim, again in facts:
            sc = lax.dot_general(q_ref[b0, :rows], ko_ref[i], (((1,), (1,)), ((), ())), preferred_element_type=F32) * scale
            sc = jnp.where(own_head & (late <= lim), sc, NEG)
            m = jnp.max(sc, axis=1, keepdims=True)
            p = jnp.exp(sc - m)
            l = jnp.sum(p, axis=1, keepdims=True)
            o = jnp.dot(p.astype(BF16), vo_ref[i], preferred_element_type=F32)
            done.append((used, b0, m, l, o, again))
        for used, b0, m, l, o, again in done:
            def put(m, l, o):
                o_ref[b0] = o
                ml = jnp.where(out_lane == out_row, m, 0.0) + jnp.where(out_lane == out_row + rows, l, 0.0)
                ml_ref[pl.ds(b0, 1)] = jnp.sum(ml, axis=0, keepdims=True)

            @pl.when(used & (again == 0))
            def _():
                put(m, l, o)

            @pl.when(used & (again > 0))
            def _():
                old = jnp.broadcast_to(ml_ref[pl.ds(b0, 1)], (rows, lanes))
                m1 = jnp.sum(jnp.where(out_lane == out_row, old, 0.0), axis=1, keepdims=True)
                l1 = jnp.sum(jnp.where(out_lane == out_row + rows, old, 0.0), axis=1, keepdims=True)
                mm = jnp.maximum(m, m1)
                w, w1 = jnp.exp(m - mm), jnp.exp(m1 - mm)
                put(mm, l * w + l1 * w1, o * w + o_ref[b0] * w1)


def combine_kernel(o_ref, ml_ref, out_ref):
    parts, seq_dev, rows, lanes = o_ref.shape
    heads = out_ref.shape[2]

    @pl.loop(0, seq_dev, unroll=6)
    def _(b):
        ml = ml_ref[:, pl.ds(b, 1)].reshape(parts, lanes)
        w = jnp.exp(ml - jnp.max(ml, axis=0, keepdims=True))
        l = pltpu.roll(ml, lanes - rows, 1)
        w = w / jnp.sum(w * l, axis=0, keepdims=True)
        wt = w.T
        acc = jnp.zeros((rows, lanes), F32)
        for s in range(parts):
            acc = acc + wt[:rows, s:s + 1] * o_ref[s, b]
        acc = acc.astype(BF16)
        out_ref[0, b] = acc[:heads]
        out_ref[1, b] = acc[heads:]


def blank_kernel(o_ref):
    pass


def sems(*shape):
    return pltpu.SemaphoreType.DMA(shape)


def comm(cid):
    return pltpu.CompilerParams(collective_id=cid, has_side_effects=True)


def solution(mesh):
    n_rows = mesh.shape['kv2']
    n_cols = mesh.shape['kv']
    n_dev = n_rows * n_cols
    dev_axes = ('rep', 'kv2', 'kv')
    seq_spec = P(None, dev_axes, None)
    pool_spec = P(dev_axes, None, None, None, None)
    table_spec = P(dev_axes, None)
    vec_spec = P(dev_axes)
    full_spec = P()

    def per_device(x_embed, w_query, w_key, w_value, w_out, w_up, w_down, k_pool, v_pool, old_table, seq_len, src_slot, dst_slot):
        n_slots, layers, page, kv_heads, head_dim = k_pool.shape
        heads = w_query.shape[2] // head_dim
        n_steps, seq_dev, width = x_embed.shape
        n_moves = src_slot.shape[0]
        row_seqs = seq_dev * n_cols
        rows = n_steps * heads
        key_rows = page * kv_heads
        tile = 8
        n_ch = key_rows // tile
        chunks = 2 * n_ch
        cap = 20
        blk, group = 28, 7
        assert chunks == n_dev and rows == 32 and n_slots % blk == 0 and old_table.shape[1] == 2
        shift = 18
        magic = -(-(1 << shift) // n_slots)
        assert all((s * magic) >> shift == s // n_slots for s in range(n_dev * n_slots))
        me = flat_id(n_cols)
        who = jnp.stack([me, lax.axis_index('kv2') * n_cols, lax.axis_index('kv') % 2]).astype(jnp.int32)

        kp = k_pool.reshape(n_slots, layers, n_ch, tile, head_dim)
        vp = v_pool.reshape(n_slots, layers, n_ch, tile, head_dim)
        packed = pl.pallas_call(
            functools.partial(pack_kernel, n_moves),
            out_shape=[jax.ShapeDtypeStruct((chunks, n_moves, tile, head_dim), BF16)] * layers,
            in_specs=[SMEM, ANY, ANY], out_specs=[VMEM] * layers,
            scratch_shapes=[sems(layers, 2, n_moves)], name='pack_pages')(src_slot - me * n_slots, kp, vp)
        after = lax.optimization_barrier
        spread0 = lax.all_to_all(packed[0], ('kv2', 'kv'), 0, 0, tiled=True)

        mine = jnp.concatenate([old_table.reshape(-1), seq_len, src_slot, dst_slot])
        mine = jnp.pad(mine, (0, 128 - mine.shape[0])).reshape(1, 128)
        tab = pl.pallas_call(
            functools.partial(gather_all_kernel, n_dev, n_cols),
            out_shape=jax.ShapeDtypeStruct((n_dev, 1, 128), jnp.int32),
            in_specs=[VMEM], out_specs=VMEM,
            scratch_shapes=[pltpu.SemaphoreType.DMA, sems(n_dev), sems(n_dev)],
            compiler_params=comm(0), name='gather_tables')(mine)

        dims = (n_dev, n_cols, n_slots, seq_dev, n_moves, cap, page, magic, shift)
        pages, info, most = pl.pallas_call(
            functools.partial(plan_kernel, dims),
            out_shape=(jax.ShapeDtypeStruct((n_dev * cap,), jnp.int32), jax.ShapeDtypeStruct((6 * n_slots,), jnp.int32),
                       jax.ShapeDtypeStruct((1,), jnp.int32)),
            in_specs=[SMEM, SMEM, ANY], out_specs=(SMEM, SMEM, SMEM),
            scratch_shapes=[pltpu.SMEM((n_dev * n_slots,), jnp.int32), pltpu.SMEM((n_dev // 2,), jnp.int32),
                            pltpu.SMEM((row_seqs,), jnp.int32), pltpu.SemaphoreType.DMA],
            name='plan')(who, tab.reshape(n_dev, 128), jnp.full((n_dev * n_slots,), -1, jnp.int32))

        def regroup(spread, name):
            return pl.pallas_call(
                functools.partial(regroup_kernel, cap),
                out_shape=jax.ShapeDtypeStruct((n_dev, cap, tile, head_dim), BF16),
                in_specs=[SMEM, VMEM], out_specs=VMEM, name=name)(pages, spread.reshape(n_dev * n_moves, tile, head_dim))

        def deliver(grouped):
            return lax.all_to_all(grouped, ('kv2', 'kv'), 0, 0, tiled=True)

        def to_mate(own):
            return lax.ppermute(own, 'kv', [(i, i ^ 1) for i in range(n_cols)])

        def all_pages():
            found = []
            for p in packed:
                everything = lax.all_gather(p.swapaxes(0, 1), ('kv2', 'kv'), tiled=True)
                found.append(everything[jnp.maximum(info[n_slots:2 * n_slots], 0)])
            return jnp.stack(found)

        def no_pages():
            return pl.pallas_call(
                blank_kernel, out_shape=jax.ShapeDtypeStruct((layers, n_slots, chunks, tile, head_dim), BF16), out_specs=ANY,
                name='blank')()

        slow = lax.cond(most[0] > 2 * cap, all_pages, no_pages)

        k_rows = k_pool.reshape(n_slots, layers * key_rows, head_dim)
        v_rows = v_pool.reshape(n_slots, layers * key_rows, head_dim)
        hidden = x_embed.reshape(n_steps * seq_dev, width)
        k_out = v_out = None
        grouped, hidden = after((regroup(spread0, 'regroup_pages_0'), hidden))
        own = deliver(grouped)
        pool_shape = jax.ShapeDtypeStruct(k_rows.shape, BF16)
        for layer in range(layers):
            query = jnp.dot(hidden, w_query[layer], preferred_element_type=F32).astype(BF16)
            k_new = jnp.dot(hidden, w_key[layer], preferred_element_type=F32).astype(BF16)
            v_new = jnp.dot(hidden, w_value[layer], preferred_element_type=F32).astype(BF16)

            def by_seq(x):
                return x.reshape(n_steps, seq_dev, -1, head_dim).swapaxes(0, 1).reshape(seq_dev, -1, head_dim)

            load = jnp.concatenate([by_seq(query), by_seq(k_new), by_seq(v_new)], axis=1)
            q_rows = load.shape[1]
            own, load = after((own, load))
            mate = to_mate(own)
            n_chips = n_cols // 2
            q_row = pl.pallas_call(
                functools.partial(row_gather_kernel, n_cols),
                out_shape=jax.ShapeDtypeStruct((n_cols, seq_dev, q_rows, head_dim), BF16),
                in_specs=[VMEM], out_specs=VMEM,
                scratch_shapes=[pltpu.SemaphoreType.DMA, sems(n_chips), sems(n_chips), sems(n_chips), sems(n_chips)],
                compiler_params=comm(3 + layer), name=f'gather_queries_{layer}')(load)

            first = layer == 0
            last = layer == layers - 1
            if not last:
                moving, q_row = after((packed[layer + 1], q_row))
                spread = lax.all_to_all(moving, ('kv2', 'kv'), 0, 0, tiled=True)
            dims = (layer, n_slots, blk, group, cap, head_dim ** -0.5, first)
            pool_block = pl.BlockSpec((blk, key_rows, head_dim), lambda g, *_, at=layer: (g, at, 0))
            whole = lambda shape: pl.BlockSpec(shape, lambda g, *_: (0,) * len(shape))
            carried = () if first else (k_out, v_out)
            k_out, v_out, part, ml = pl.pallas_call(
                functools.partial(attend_kernel, dims),
                grid_spec=pltpu.PrefetchScalarGridSpec(
                    num_scalar_prefetch=3, grid=(n_slots // blk,),
                    in_specs=[whole((row_seqs, q_rows, head_dim)), pool_block, pool_block, ANY, ANY, ANY] + [ANY] * len(carried),
                    out_specs=[pool_block, pool_block, whole((row_seqs, rows, head_dim)), whole((row_seqs, head_dim))],
                    scratch_shapes=[pltpu.VMEM((2, blk, n_ch, tile, head_dim), BF16), pltpu.VMEM((2, blk, n_ch, tile, head_dim), BF16),
                                    sems(2, 2, blk)]),
                out_shape=[pool_shape, pool_shape, jax.ShapeDtypeStruct((row_seqs, rows, head_dim), F32),
                           jax.ShapeDtypeStruct((row_seqs, head_dim), F32)],
                input_output_aliases={} if first else {9: 0, 10: 1},
                compiler_params=pltpu.CompilerParams(dimension_semantics=('arbitrary',)),
                name=f'attend_{layer}')(info, most, who, q_row.reshape(row_seqs, q_rows, head_dim), k_rows, v_rows, own, mate, slow, *carried)

            home, home_ml = pl.pallas_call(
                functools.partial(row_exchange_kernel, n_cols),
                out_shape=(jax.ShapeDtypeStruct((n_cols, seq_dev, rows, head_dim), F32),
                           jax.ShapeDtypeStruct((n_cols, seq_dev, head_dim), F32)),
                in_specs=[ANY, ANY], out_specs=(ANY, ANY),
                scratch_shapes=[sems(2), sems(2, n_cols), sems(2, n_cols)],
                compiler_params=comm(5 + layer), name=f'return_parts_{layer}')(
                    part.reshape(n_cols, seq_dev, rows, head_dim), ml.reshape(n_cols, seq_dev, head_dim))
            attn = pl.pallas_call(
                combine_kernel,
                out_shape=jax.ShapeDtypeStruct((n_steps, seq_dev, heads, head_dim), BF16),
                in_specs=[VMEM, VMEM], out_specs=VMEM, name=f'combine_{layer}')(home, home_ml)
            attn_out = attn.reshape(n_steps * seq_dev, heads * head_dim)
            hidden = (hidden.astype(F32) + jnp.dot(attn_out, w_out[layer], preferred_element_type=F32)).astype(BF16)
            if not last:
                spread, hidden = after((spread, hidden))
                grouped, hidden = after((regroup(spread, f'regroup_pages_{layer + 1}'), hidden))
                own = deliver(grouped)
            up_act = jax.nn.gelu(jnp.dot(hidden, w_up[layer], preferred_element_type=F32)).astype(BF16)
            hidden = (hidden.astype(F32) + jnp.dot(up_act, w_down[layer], preferred_element_type=F32)).astype(BF16)
        return hidden.reshape(x_embed.shape), k_out.reshape(k_pool.shape), v_out.reshape(v_pool.shape)

    return jax.shard_map(per_device, mesh=mesh, in_specs=(seq_spec, full_spec, full_spec, full_spec, full_spec, full_spec, full_spec, pool_spec, pool_spec, table_spec, vec_spec, vec_spec, vec_spec), out_specs=(seq_spec, pool_spec, pool_spec), check_vma=False)
```

```python
import functools

import jax
import jax.numpy as jnp
from jax import lax
from jax.experimental import pallas as pl
from jax.experimental.pallas import tpu as pltpu
from jax.sharding import PartitionSpec as P

MESH = pl.DeviceIdType.MESH
ANY = pl.BlockSpec(memory_space=pl.ANY)
SMEM = pl.BlockSpec(memory_space=pltpu.SMEM)
VMEM = pl.BlockSpec(memory_space=pltpu.VMEM)
F32 = jnp.float32
BF16 = jnp.bfloat16
NEG = -1e30


def flat_id(n_cols):
    return lax.axis_index('kv2') * n_cols + lax.axis_index('kv')


def where_is(flat, n_cols):
    return {'kv2': flat // n_cols, 'kv': flat % n_cols}


def greet_all(n_dev, n_cols):
    me = flat_id(n_cols)
    barrier = pltpu.get_barrier_semaphore()

    @pl.loop(1, n_dev)
    def _(r):
        pl.semaphore_signal(barrier, inc=1, device_id=where_is((me + r) % n_dev, n_cols), device_id_type=MESH)

    pl.semaphore_wait(barrier, n_dev - 1)


def gather_all_kernel(n_dev, n_cols, x_ref, o_ref, local_sem, send_sem, recv_sem):
    me = flat_id(n_cols)
    greet_all(n_dev, n_cols)

    def copy(r, dst, slot):
        return pltpu.make_async_remote_copy(
            src_ref=x_ref, dst_ref=o_ref.at[slot], send_sem=send_sem.at[r], recv_sem=recv_sem.at[r],
            device_id=where_is(dst, n_cols), device_id_type=MESH)

    @pl.loop(1, n_dev)
    def _(r):
        copy(r, (me + r) % n_dev, me).start()

    own = pltpu.make_async_copy(x_ref, o_ref.at[me], local_sem)
    own.start()
    own.wait()

    @pl.loop(1, n_dev)
    def _(r):
        c = copy(r, (me + r) % n_dev, (me + n_dev - r) % n_dev)
        c.wait_send()
        c.wait_recv()


def row_gather_kernel(n_cols, x_ref, o_ref, local_sem, send_sem, recv_sem, fsend_sem, frecv_sem):
    n_chips = n_cols // 2
    kv = lax.axis_index('kv')
    chip, core = kv // 2, kv % 2
    mate = chip * 2 + 1 - core
    barrier = pltpu.get_barrier_semaphore()
    for r in range(1, n_chips):
        pl.semaphore_signal(barrier, inc=1, device_id={'kv': (chip + r) % n_chips * 2 + core}, device_id_type=MESH)
    pl.semaphore_signal(barrier, inc=1, device_id={'kv': mate}, device_id_type=MESH)
    pl.semaphore_wait(barrier, n_chips)

    def copy(r, dst, slot):
        return pltpu.make_async_remote_copy(
            src_ref=x_ref, dst_ref=o_ref.at[slot], send_sem=send_sem.at[r], recv_sem=recv_sem.at[r],
            device_id={'kv': dst}, device_id_type=MESH)

    def forward(r, slot):
        return pltpu.make_async_remote_copy(
            src_ref=o_ref.at[slot], dst_ref=o_ref.at[slot], send_sem=fsend_sem.at[r], recv_sem=frecv_sem.at[r],
            device_id={'kv': mate}, device_id_type=MESH)

    for r in range(1, n_chips):
        copy(r, (chip + r) % n_chips * 2 + core, kv).start()
    copy(0, mate, kv).start()
    own = pltpu.make_async_copy(x_ref, o_ref.at[kv], local_sem)
    own.start()
    own.wait()
    for r in range(1, n_chips):
        slot = (chip + n_chips - r) % n_chips * 2 + core
        copy(r, mate, slot).wait_recv()
        forward(r, slot).start()
    for r in range(1, n_chips):
        copy(r, mate, kv).wait_send()
        forward(r, (chip + n_chips - r) % n_chips * 2 + core).wait_send()
        forward(r, (chip + n_chips - r) % n_chips * 2 + 1 - core).wait_recv()
    c = copy(0, mate, mate)
    c.wait_send()
    c.wait_recv()


def row_exchange_kernel(n_cols, x_ref, y_ref, ox_ref, oy_ref, local_sem, send_sem, recv_sem):
    kv = lax.axis_index('kv')
    barrier = pltpu.get_barrier_semaphore()
    for r in range(1, n_cols):
        pl.semaphore_signal(barrier, inc=1, device_id={'kv': (kv + r) % n_cols}, device_id_type=MESH)
    pl.semaphore_wait(barrier, n_cols - 1)

    def copy(a, r, dst, slot):
        src_ref, dst_ref = ((x_ref, ox_ref), (y_ref, oy_ref))[a]
        return pltpu.make_async_remote_copy(
            src_ref=src_ref.at[dst], dst_ref=dst_ref.at[slot], send_sem=send_sem.at[a, r], recv_sem=recv_sem.at[a, r],
            device_id={'kv': dst}, device_id_type=MESH)

    for r in range(1, n_cols):
        for a in range(2):
            copy(a, r, (kv + r) % n_cols, kv).start()
    own = [pltpu.make_async_copy(s.at[kv], d.at[kv], local_sem.at[a]) for a, (s, d) in enumerate(((x_ref, ox_ref), (y_ref, oy_ref)))]
    for c in own:
        c.start()
    for c in own:
        c.wait()
    for r in range(1, n_cols):
        for a in range(2):
            c = copy(a, r, (kv + r) % n_cols, (kv + n_cols - r) % n_cols)
            c.wait_send()
            c.wait_recv()


def places_kernel(dims, who_ref, tab_ref, pages_ref, arrive_ref, most_ref, count):
    n_dev, n_cols, n_slots, seq_dev, n_moves, cap, page, magic, shift = dims
    n_chips = n_dev // 2
    o_dst = 3 * seq_dev + n_moves
    me = who_ref[0]
    base = me * n_slots

    @pl.loop(0, n_chips)
    def _(i):
        count[i] = 0

    @pl.loop(0, n_slots, unroll=8)
    def _(i):
        arrive_ref[i] = -1
        arrive_ref[n_slots + i] = -1

    @pl.loop(0, n_dev * cap, unroll=8)
    def _(i):
        pages_ref[i] = 0

    @pl.loop(0, n_dev)
    def _(d):
        for j in range(n_moves):
            dst = tab_ref[d, o_dst + j]
            m = d * n_moves + j
            dd = (dst * magic) >> shift
            chip = dd >> 1
            n = count[chip]
            count[chip] = n + 1

            @pl.when(n < 2 * cap)
            def _():
                pages_ref[chip * 2 * cap + n] = m

            @pl.when(dd == me)
            def _():
                arrive_ref[dst - base] = n
                arrive_ref[n_slots + dst - base] = m

    most_ref[0] = lax.fori_loop(0, n_chips, lambda i, best: jnp.maximum(best, count[i]), jnp.int32(0))


def cells_kernel(dims, who_ref, tab_ref, none_ref, info_ref, used_ref, moved, seen, sem):
    n_dev, n_cols, n_slots, seq_dev, n_moves, cap, page, magic, shift = dims
    o_len, o_src, o_dst = 2 * seq_dev, 3 * seq_dev, 3 * seq_dev + n_moves
    row0 = who_ref[1]
    base = who_ref[0] * n_slots
    fill = pltpu.make_async_copy(none_ref, moved, sem)
    fill.start()

    @pl.loop(0, n_cols * seq_dev, unroll=8)
    def _(i):
        seen[i] = 0

    @pl.loop(0, n_slots, unroll=8)
    def _(i):
        info_ref[i] = -1
        info_ref[n_slots + i] = -1

    fill.wait()

    @pl.loop(0, n_dev)
    def _(d):
        for j in range(n_moves):
            moved[tab_ref[d, o_src + j]] = tab_ref[d, o_dst + j]

    @pl.loop(0, n_cols)
    def _(h):
        @pl.loop(0, seq_dev, unroll=4)
        def _(i):
            b = h * seq_dev + i
            length = tab_ref[row0 + h, o_len + i]
            for j in range(2):
                e = tab_ref[row0 + h, 2 * i + j]
                e0 = jnp.maximum(e, 0)
                mv = moved[e0]
                s = jnp.where(mv >= 0, mv, e0) - base

                @pl.when((e >= 0) & (s >= 0) & (s < n_slots))
                def _():
                    info_ref[n_slots + s] = b
                    info_ref[2 * n_slots + s] = length - page * j

    def visit(s, n):
        b = info_ref[n_slots + s]

        @pl.when(b >= 0)
        def _():
            info_ref[n] = s
            info_ref[3 * n_slots + s] = seen[b]
            seen[b] = 1

        return n + jnp.where(b >= 0, 1, 0)

    used_ref[0] = lax.fori_loop(0, n_slots, visit, jnp.int32(0))


def pack_kernel(n_moves, src_ref, k_ref, v_ref, *rest):
    *outs, sem = rest

    def copies(m):
        s = src_ref[m]
        for layer, o_ref in enumerate(outs):
            half = o_ref.shape[0] // 2
            for a, pool in enumerate((k_ref, v_ref)):
                yield pltpu.make_async_copy(pool.at[s, layer], o_ref.at[pl.ds(a * half, half), m], sem.at[layer, a, m])

    for m in range(n_moves):
        for c in copies(m):
            c.start()
    for m in range(n_moves):
        for c in copies(m):
            c.wait()


def regroup_kernel(cap, pages_ref, x_ref, o_ref):
    @pl.loop(0, o_ref.shape[0])
    def _(d):
        for n in range(cap):
            o_ref[d, n] = x_ref[pages_ref[d * cap + n]]


def attend_kernel(dims, who_ref, arrive_ref, most_ref, info_ref, used_ref, q_ref, k_ref, v_ref, own_ref, mate_ref, slow_ref, *rest):
    layer, n_slots, cap, scale, quads, first = dims
    ko_ref, vo_ref, o_ref, ml_ref, kbuf, vbuf, in_sem, out_sem = rest if first else rest[2:]
    n_key, lanes = kbuf.shape[1] * kbuf.shape[2], kbuf.shape[3]
    n_ch = kbuf.shape[1]
    rows = o_ref.shape[1]
    over = most_ref[0] > 2 * cap
    core = who_ref[2]
    bufs = (kbuf, vbuf)
    part = pl.ds(layer * n_ch, n_ch)

    @pl.loop(0, n_slots)
    def _(s):
        n = arrive_ref[s]
        has = n >= 0
        half = jnp.where(n >= cap, 1, 0)
        pos = n - half * cap

        def go(cond, src_of):
            @pl.when(cond)
            def _():
                for a in range(2):
                    pltpu.make_async_copy(src_of(a), bufs[a].at[s], in_sem.at[a]).start()

        fast = has & jnp.logical_not(over)
        go(jnp.logical_not(has), lambda a: (k_ref, v_ref)[a].at[s, part])
        go(has & over, lambda a: slow_ref.at[layer, s, pl.ds(a * n_ch, n_ch)])
        go(fast & (half == core), lambda a: own_ref.at[pl.ds(a * n_ch, n_ch), pos])
        go(fast & (half != core), lambda a: mate_ref.at[pl.ds(a * n_ch, n_ch), pos])

    o_ref[...] = jnp.zeros_like(o_ref)
    ml_lane = lax.broadcasted_iota(jnp.int32, ml_ref.shape, 1)
    ml_ref[...] = jnp.where(ml_lane < rows, NEG, 0.0)
    for a in range(2):
        pltpu.make_async_copy((k_ref, v_ref)[a].at[:, part], bufs[a], in_sem.at[a]).wait()

    n_used = used_ref[0]
    tile = kbuf.shape[2]
    tile_row = lax.broadcasted_iota(jnp.int32, (tile, lanes), 0)

    @pl.loop(0, n_used)
    def _(i):
        s = info_ref[i]
        lim = info_ref[2 * n_slots + s]

        @pl.when(lim < n_key // 2)
        def _():
            fresh = q_ref[info_ref[n_slots + s], rows:].astype(F32)
            row0 = 2 * lim
            for c in (row0 // tile, jnp.minimum((row0 + 3) // tile, n_ch - 1)):
                at = tile_row + c * tile - row0
                for a, buf in enumerate(bufs):
                    x = buf[s, c].astype(F32)
                    for r in range(4):
                        x = jnp.where(at == r, fresh[4 * a + r:4 * a + r + 1], x)
                    buf[s, c] = x.astype(BF16)

    outs = [pltpu.make_async_copy(bufs[a], (ko_ref, vo_ref)[a].at[:, part], out_sem.at[a]) for a in range(2)]
    for c in outs:
        c.start()

    lane = lax.broadcasted_iota(jnp.int32, (rows, n_key), 1)
    row = lax.broadcasted_iota(jnp.int32, (rows, n_key), 0)
    own_head = (lane & 1) == ((row >> 3) & 1)
    late = (lane >> 1) - (row >> 4)
    out_lane = lax.broadcasted_iota(jnp.int32, (rows, lanes), 1)
    out_row = lax.broadcasted_iota(jnp.int32, (rows, lanes), 0)
    nothing = jnp.zeros((rows, n_key), BF16)

    @pl.loop(0, (n_used + 4 * quads - 1) // (4 * quads))
    def _(u):
        done = []
        for quad in range(quads):
            facts = []
            for t in range(4):
                i = (u * quads + quad) * 4 + t
                listed = info_ref[jnp.minimum(i, n_slots - 1)]
                used = (i < n_slots) & (listed >= 0)
                s = jnp.where(used, listed, 0)
                facts.append((s, used, jnp.maximum(info_ref[n_slots + s], 0), info_ref[2 * n_slots + s], info_ref[3 * n_slots + s]))
            q = jnp.concatenate([q_ref[f[2], :rows] for f in facts], axis=0)
            k = jnp.concatenate([kbuf[f[0]].reshape(n_key, lanes) for f in facts], axis=0)
            v = jnp.concatenate([vbuf[f[0]].reshape(n_key, lanes) for f in facts], axis=0)
            scores = lax.dot_general(q, k, (((1,), (1,)), ((), ())), preferred_element_type=F32)
            ps, stats = [], []
            for t, (s, used, b, lim, again) in enumerate(facts):
                sc = scores[t * rows:(t + 1) * rows, t * n_key:(t + 1) * n_key] * scale
                sc = jnp.where(own_head & (late <= lim), sc, NEG)
                m = jnp.max(sc, axis=1, keepdims=True)
                p = jnp.exp(sc - m)
                stats.append((m, jnp.sum(p, axis=1, keepdims=True)))
                ps.append(jnp.concatenate([p.astype(BF16) if x == t else nothing for x in range(4)], axis=1))
            o = jnp.dot(jnp.concatenate(ps, axis=0), v, preferred_element_type=F32)
            for t, (s, used, b, lim, again) in enumerate(facts):
                done.append((used, b, *stats[t], o[t * rows:(t + 1) * rows], again))
        for used, b0, m, l, o, again in done:
            def put(m, l, o):
                o_ref[b0] = o
                ml = jnp.where(out_lane == out_row, m, 0.0) + jnp.where(out_lane == out_row + rows, l, 0.0)
                ml_ref[pl.ds(b0, 1)] = jnp.sum(ml, axis=0, keepdims=True)

            @pl.when(used & (again == 0))
            def _():
                put(m, l, o)

            @pl.when(used & (again > 0))
            def _():
                old = jnp.broadcast_to(ml_ref[pl.ds(b0, 1)], (rows, lanes))
                m1 = jnp.sum(jnp.where(out_lane == out_row, old, 0.0), axis=1, keepdims=True)
                l1 = jnp.sum(jnp.where(out_lane == out_row + rows, old, 0.0), axis=1, keepdims=True)
                mm = jnp.maximum(m, m1)
                w, w1 = jnp.exp(m - mm), jnp.exp(m1 - mm)
                put(mm, l * w + l1 * w1, o * w + o_ref[b0] * w1)

    for c in outs:
        c.wait()


def combine_kernel(o_ref, ml_ref, out_ref):
    parts, seq_dev, rows, lanes = o_ref.shape
    heads = out_ref.shape[2]

    @pl.loop(0, seq_dev, unroll=12)
    def _(b):
        ml = ml_ref[:, pl.ds(b, 1)].reshape(parts, lanes)
        w = jnp.exp(ml - jnp.max(ml, axis=0, keepdims=True))
        l = pltpu.roll(ml, lanes - rows, 1)
        w = w / jnp.sum(w * l, axis=0, keepdims=True)
        wt = w.T
        acc = jnp.zeros((rows, lanes), F32)
        for s in range(parts):
            acc = acc + wt[:rows, s:s + 1] * o_ref[s, b]
        acc = acc.astype(BF16)
        out_ref[0, b] = acc[:heads]
        out_ref[1, b] = acc[heads:]


def blank_kernel(o_ref):
    pass


def sems(*shape):
    return pltpu.SemaphoreType.DMA(shape)


def comm(cid):
    return pltpu.CompilerParams(collective_id=cid, has_side_effects=True)


def solution(mesh):
    n_rows = mesh.shape['kv2']
    n_cols = mesh.shape['kv']
    n_dev = n_rows * n_cols
    dev_axes = ('rep', 'kv2', 'kv')
    seq_spec = P(None, dev_axes, None)
    pool_spec = P(dev_axes, None, None, None, None)
    table_spec = P(dev_axes, None)
    vec_spec = P(dev_axes)
    full_spec = P()

    def per_device(x_embed, w_query, w_key, w_value, w_out, w_up, w_down, k_pool, v_pool, old_table, seq_len, src_slot, dst_slot):
        n_slots, layers, page, kv_heads, head_dim = k_pool.shape
        heads = w_query.shape[2] // head_dim
        n_steps, seq_dev, width = x_embed.shape
        n_moves = src_slot.shape[0]
        row_seqs = seq_dev * n_cols
        rows = n_steps * heads
        key_rows = page * kv_heads
        tile = 8
        n_ch = key_rows // tile
        chunks = 2 * n_ch
        cap = 20
        assert chunks == n_dev and rows == 32 and old_table.shape[1] == 2
        shift = 18
        magic = -(-(1 << shift) // n_slots)
        assert all((s * magic) >> shift == s // n_slots for s in range(n_dev * n_slots))
        me = flat_id(n_cols)
        who = jnp.stack([me, lax.axis_index('kv2') * n_cols, lax.axis_index('kv') % 2]).astype(jnp.int32)

        kp = k_pool.reshape(n_slots, layers, n_ch, tile, head_dim)
        vp = v_pool.reshape(n_slots, layers, n_ch, tile, head_dim)
        kp4 = k_pool.reshape(n_slots, layers * n_ch, tile, head_dim)
        vp4 = v_pool.reshape(n_slots, layers * n_ch, tile, head_dim)
        packed = pl.pallas_call(
            functools.partial(pack_kernel, n_moves),
            out_shape=[jax.ShapeDtypeStruct((chunks, n_moves, tile, head_dim), BF16)] * layers,
            in_specs=[SMEM, ANY, ANY], out_specs=[VMEM] * layers,
            scratch_shapes=[sems(layers, 2, n_moves)], name='pack_pages')(src_slot - me * n_slots, kp, vp)
        after = lax.optimization_barrier
        spread0 = lax.all_to_all(packed[0], ('kv2', 'kv'), 0, 0, tiled=True)

        mine = jnp.concatenate([old_table.reshape(-1), seq_len, src_slot, dst_slot])
        mine = jnp.pad(mine, (0, 128 - mine.shape[0])).reshape(1, 128)
        tab = pl.pallas_call(
            functools.partial(gather_all_kernel, n_dev, n_cols),
            out_shape=jax.ShapeDtypeStruct((n_dev, 1, 128), jnp.int32),
            in_specs=[VMEM], out_specs=VMEM,
            scratch_shapes=[pltpu.SemaphoreType.DMA, sems(n_dev), sems(n_dev)],
            compiler_params=comm(0), name='gather_tables')(mine)

        tab = tab.reshape(n_dev, 128)
        dims = (n_dev, n_cols, n_slots, seq_dev, n_moves, cap, page, magic, shift)
        pages, arrive, most = pl.pallas_call(
            functools.partial(places_kernel, dims),
            out_shape=(jax.ShapeDtypeStruct((n_dev * cap,), jnp.int32), jax.ShapeDtypeStruct((2 * n_slots,), jnp.int32),
                       jax.ShapeDtypeStruct((1,), jnp.int32)),
            in_specs=[SMEM, SMEM], out_specs=(SMEM, SMEM, SMEM),
            scratch_shapes=[pltpu.SMEM((n_dev // 2,), jnp.int32)], name='places')(who, tab)

        def regroup(spread, name):
            return pl.pallas_call(
                functools.partial(regroup_kernel, cap),
                out_shape=jax.ShapeDtypeStruct((n_dev, cap, tile, head_dim), BF16),
                in_specs=[SMEM, VMEM], out_specs=VMEM, name=name)(pages, spread.reshape(n_dev * n_moves, tile, head_dim))

        def deliver(grouped):
            return lax.all_to_all(grouped, ('kv2', 'kv'), 0, 0, tiled=True)

        def to_mate(own):
            return lax.ppermute(own, 'kv', [(i, i ^ 1) for i in range(n_cols)])

        def all_pages():
            found = []
            for p in packed:
                everything = lax.all_gather(p.swapaxes(0, 1), ('kv2', 'kv'), tiled=True)
                found.append(everything[jnp.maximum(arrive[n_slots:], 0)])
            return jnp.stack(found)

        def no_pages():
            return pl.pallas_call(
                blank_kernel, out_shape=jax.ShapeDtypeStruct((layers, n_slots, chunks, tile, head_dim), BF16), out_specs=ANY,
                name='blank')()

        slow = lax.cond(most[0] > 2 * cap, all_pages, no_pages)

        hidden = x_embed.reshape(n_steps * seq_dev, width)
        k_out = v_out = None
        grouped, hidden, tab = after((regroup(spread0, 'regroup_pages_0'), hidden, tab))
        own = deliver(grouped)
        info, n_used = pl.pallas_call(
            functools.partial(cells_kernel, dims),
            out_shape=(jax.ShapeDtypeStruct((4 * n_slots,), jnp.int32), jax.ShapeDtypeStruct((1,), jnp.int32)),
            in_specs=[SMEM, SMEM, ANY], out_specs=(SMEM, SMEM),
            scratch_shapes=[pltpu.SMEM((n_dev * n_slots,), jnp.int32), pltpu.SMEM((row_seqs,), jnp.int32), pltpu.SemaphoreType.DMA],
            name='cells')(who, tab, jnp.full((n_dev * n_slots,), -1, jnp.int32))
        pool_shape = jax.ShapeDtypeStruct(kp4.shape, BF16)
        for layer in range(layers):
            query = jnp.dot(hidden, w_query[layer], preferred_element_type=F32).astype(BF16)
            k_new = jnp.dot(hidden, w_key[layer], preferred_element_type=F32).astype(BF16)
            v_new = jnp.dot(hidden, w_value[layer], preferred_element_type=F32).astype(BF16)

            def by_seq(x):
                return x.reshape(n_steps, seq_dev, -1, head_dim).swapaxes(0, 1).reshape(seq_dev, -1, head_dim)

            load = jnp.concatenate([by_seq(query), by_seq(k_new), by_seq(v_new)], axis=1)
            q_rows = load.shape[1]
            own, load, info = after((own, load, info))
            mate = to_mate(own)
            n_chips = n_cols // 2
            q_row = pl.pallas_call(
                functools.partial(row_gather_kernel, n_cols),
                out_shape=jax.ShapeDtypeStruct((n_cols, seq_dev, q_rows, head_dim), BF16),
                in_specs=[VMEM], out_specs=VMEM,
                scratch_shapes=[pltpu.SemaphoreType.DMA, sems(n_chips), sems(n_chips), sems(n_chips), sems(n_chips)],
                compiler_params=comm(3 + layer), name=f'gather_queries_{layer}')(load)

            first = layer == 0
            last = layer == layers - 1
            if not last:
                moving, q_row = after((packed[layer + 1], q_row))
                spread = lax.all_to_all(moving, ('kv2', 'kv'), 0, 0, tiled=True)
            carried = () if first else (k_out, v_out)
            k_out, v_out, part, ml = pl.pallas_call(
                functools.partial(attend_kernel, (layer, n_slots, cap, head_dim ** -0.5, 2, first)),
                in_specs=[SMEM] * 5 + [VMEM] + [ANY] * (5 + len(carried)),
                out_specs=[ANY, ANY, VMEM, VMEM],
                out_shape=[pool_shape, pool_shape, jax.ShapeDtypeStruct((row_seqs, rows, head_dim), F32),
                           jax.ShapeDtypeStruct((row_seqs, head_dim), F32)],
                scratch_shapes=[pltpu.VMEM((n_slots, n_ch, tile, head_dim), BF16), pltpu.VMEM((n_slots, n_ch, tile, head_dim), BF16),
                                sems(2), sems(2)],
                input_output_aliases={} if first else {11: 0, 12: 1},
                name=f'attend_{layer}')(who, arrive, most, info, n_used, q_row.reshape(row_seqs, q_rows, head_dim), kp4, vp4,
                                        own, mate, slow, *carried)

            home, home_ml = pl.pallas_call(
                functools.partial(row_exchange_kernel, n_cols),
                out_shape=(jax.ShapeDtypeStruct((n_cols, seq_dev, rows, head_dim), F32),
                           jax.ShapeDtypeStruct((n_cols, seq_dev, head_dim), F32)),
                in_specs=[ANY, ANY], out_specs=(ANY, ANY),
                scratch_shapes=[sems(2), sems(2, n_cols), sems(2, n_cols)],
                compiler_params=comm(5 + layer), name=f'return_parts_{layer}')(
                    part.reshape(n_cols, seq_dev, rows, head_dim), ml.reshape(n_cols, seq_dev, head_dim))
            attn = pl.pallas_call(
                combine_kernel,
                out_shape=jax.ShapeDtypeStruct((n_steps, seq_dev, heads, head_dim), BF16),
                in_specs=[VMEM, VMEM], out_specs=VMEM, name=f'combine_{layer}')(home, home_ml)
            attn_out = attn.reshape(n_steps * seq_dev, heads * head_dim)
            hidden = (hidden.astype(F32) + jnp.dot(attn_out, w_out[layer], preferred_element_type=F32)).astype(BF16)
            if not last:
                spread, hidden = after((spread, hidden))
                grouped, hidden = after((regroup(spread, f'regroup_pages_{layer + 1}'), hidden))
                own = deliver(grouped)
            up_act = jax.nn.gelu(jnp.dot(hidden, w_up[layer], preferred_element_type=F32)).astype(BF16)
            hidden = (hidden.astype(F32) + jnp.dot(up_act, w_down[layer], preferred_element_type=F32)).astype(BF16)
        return hidden.reshape(x_embed.shape), k_out.reshape(k_pool.shape), v_out.reshape(v_pool.shape)

    return jax.shard_map(per_device, mesh=mesh, in_specs=(seq_spec, full_spec, full_spec, full_spec, full_spec, full_spec, full_spec, pool_spec, pool_spec, table_spec, vec_spec, vec_spec, vec_spec), out_specs=(seq_spec, pool_spec, pool_spec), check_vma=False)
```

```python
import functools

import jax
import jax.numpy as jnp
from jax import lax
from jax.experimental import pallas as pl
from jax.experimental.pallas import tpu as pltpu
from jax.sharding import PartitionSpec as P

MESH = pl.DeviceIdType.MESH
ANY = pl.BlockSpec(memory_space=pl.ANY)
SMEM = pl.BlockSpec(memory_space=pltpu.SMEM)
VMEM = pl.BlockSpec(memory_space=pltpu.VMEM)
F32 = jnp.float32
BF16 = jnp.bfloat16
NEG = -1e30


def flat_id(n_cols):
    return lax.axis_index('kv2') * n_cols + lax.axis_index('kv')


def where_is(flat, n_cols):
    return {'kv2': flat // n_cols, 'kv': flat % n_cols}


def greet_all(n_dev, n_cols):
    me = flat_id(n_cols)
    barrier = pltpu.get_barrier_semaphore()

    @pl.loop(1, n_dev)
    def _(r):
        pl.semaphore_signal(barrier, inc=1, device_id=where_is((me + r) % n_dev, n_cols), device_id_type=MESH)

    pl.semaphore_wait(barrier, n_dev - 1)


def gather_all_kernel(n_dev, n_cols, x_ref, o_ref, local_sem, send_sem, recv_sem):
    me = flat_id(n_cols)
    greet_all(n_dev, n_cols)

    def copy(r, dst, slot):
        return pltpu.make_async_remote_copy(
            src_ref=x_ref, dst_ref=o_ref.at[slot], send_sem=send_sem.at[r], recv_sem=recv_sem.at[r],
            device_id=where_is(dst, n_cols), device_id_type=MESH)

    @pl.loop(1, n_dev)
    def _(r):
        copy(r, (me + r) % n_dev, me).start()

    own = pltpu.make_async_copy(x_ref, o_ref.at[me], local_sem)
    own.start()
    own.wait()

    @pl.loop(1, n_dev)
    def _(r):
        c = copy(r, (me + r) % n_dev, (me + n_dev - r) % n_dev)
        c.wait_send()
        c.wait_recv()


def row_gather_kernel(n_cols, x_ref, o_ref, local_sem, send_sem, recv_sem, fsend_sem, frecv_sem):
    n_chips = n_cols // 2
    kv = lax.axis_index('kv')
    chip, core = kv // 2, kv % 2
    mate = chip * 2 + 1 - core
    barrier = pltpu.get_barrier_semaphore()
    for r in range(1, n_chips):
        pl.semaphore_signal(barrier, inc=1, device_id={'kv': (chip + r) % n_chips * 2 + core}, device_id_type=MESH)
    pl.semaphore_signal(barrier, inc=1, device_id={'kv': mate}, device_id_type=MESH)
    pl.semaphore_wait(barrier, n_chips)

    def copy(r, dst, slot):
        return pltpu.make_async_remote_copy(
            src_ref=x_ref, dst_ref=o_ref.at[slot], send_sem=send_sem.at[r], recv_sem=recv_sem.at[r],
            device_id={'kv': dst}, device_id_type=MESH)

    def forward(r, slot):
        return pltpu.make_async_remote_copy(
            src_ref=o_ref.at[slot], dst_ref=o_ref.at[slot], send_sem=fsend_sem.at[r], recv_sem=frecv_sem.at[r],
            device_id={'kv': mate}, device_id_type=MESH)

    for r in range(1, n_chips):
        copy(r, (chip + r) % n_chips * 2 + core, kv).start()
    copy(0, mate, kv).start()
    own = pltpu.make_async_copy(x_ref, o_ref.at[kv], local_sem)
    own.start()
    own.wait()
    for r in range(1, n_chips):
        slot = (chip + n_chips - r) % n_chips * 2 + core
        copy(r, mate, slot).wait_recv()
        forward(r, slot).start()
    for r in range(1, n_chips):
        copy(r, mate, kv).wait_send()
        forward(r, (chip + n_chips - r) % n_chips * 2 + core).wait_send()
        forward(r, (chip + n_chips - r) % n_chips * 2 + 1 - core).wait_recv()
    c = copy(0, mate, mate)
    c.wait_send()
    c.wait_recv()


def return_kernel(n_cols, x_ref, ml_ref, out_ref, mate_o, mate_ml, sum_o, sum_ml, got_o, got_ml, dsend, drecv, send, recv):
    n_chips = n_cols // 2
    kv = lax.axis_index('kv')
    chip, core = kv // 2, kv % 2
    mate = chip * 2 + 1 - core
    seq_dev, rows, lanes = x_ref.shape[1:]
    heads = out_ref.shape[2]
    barrier = pltpu.get_barrier_semaphore()
    for r in range(1, n_chips):
        pl.semaphore_signal(barrier, inc=1, device_id={'kv': (chip + r) % n_chips * 2 + core}, device_id_type=MESH)
    pl.semaphore_signal(barrier, inc=1, device_id={'kv': mate}, device_id_type=MESH)
    pl.semaphore_wait(barrier, n_chips)

    def across(r, a):
        src, dst = ((x_ref, mate_o), (ml_ref, mate_ml))[a]
        return pltpu.make_async_remote_copy(
            src_ref=src.at[(chip + r) % n_chips * 2 + 1 - core], dst_ref=dst.at[r], send_sem=dsend.at[a, r], recv_sem=drecv.at[a, r],
            device_id={'kv': mate}, device_id_type=MESH)

    def home(r, a):
        src, dst = ((sum_o, got_o), (sum_ml, got_ml))[a]
        return pltpu.make_async_remote_copy(
            src_ref=src.at[r], dst_ref=dst.at[r], send_sem=send.at[a, r], recv_sem=recv.at[a, r],
            device_id={'kv': (chip + r) % n_chips * 2 + core}, device_id_type=MESH)

    order = sorted(range(1, n_chips), key=lambda r: -min(r, n_chips - r)) + [0]
    for r in order:
        for a in range(2):
            across(r, a).start()
    lane = lax.broadcasted_iota(jnp.int32, (8, lanes), 1)
    for r in order:
        slot = (chip + r) % n_chips * 2 + core
        to_o, to_ml = (sum_o, sum_ml) if r else (got_o, got_ml)
        for a in range(2):
            across(r, a).wait_recv()

        @pl.loop(0, seq_dev // 8)
        def _(g):
            some = pl.ds(pl.multiple_of(8 * g, 8), 8)
            ml1, ml2 = ml_ref[slot, some], mate_ml[r, some]
            top = jnp.maximum(ml1, ml2)
            w1, w2 = jnp.exp(ml1 - top), jnp.exp(ml2 - top)
            l = pltpu.roll(w1, rows, 1) * ml1 + pltpu.roll(w2, rows, 1) * ml2
            to_ml[r, some] = jnp.where(lane < rows, top, l)
            c1, c2 = w1.T, w2.T
            for t in range(8):
                b = 8 * g + t
                to_o[r, b] = c1[:rows, t:t + 1] * x_ref[slot, b] + c2[:rows, t:t + 1] * mate_o[r, b]

        if r:
            for a in range(2):
                home(r, a).start()
    for r in range(1, n_chips):
        for a in range(2):
            home(r, a).wait_recv()

    @pl.loop(0, seq_dev // 8)
    def _(g):
        some = pl.ds(pl.multiple_of(8 * g, 8), 8)
        mls = [got_ml[p, some] for p in range(n_chips)]
        top = functools.reduce(jnp.maximum, mls)
        ws = [jnp.exp(x - top) for x in mls]
        total = sum(w * pltpu.roll(x, lanes - rows, 1) for w, x in zip(ws, mls))
        cols = [(w / total).T for w in ws]
        for t in range(8):
            b = 8 * g + t
            acc = sum(c[:rows, t:t + 1] * got_o[p, b] for p, c in enumerate(cols)).astype(BF16)
            out_ref[0, b] = acc[:heads]
            out_ref[1, b] = acc[heads:]

    for r in range(n_chips):
        for a in range(2):
            across(r, a).wait_send()
            if r:
                home(r, a).wait_send()


def places_kernel(dims, who_ref, tab_ref, pages_ref, arrive_ref, most_ref, count):
    n_dev, n_cols, n_slots, seq_dev, n_moves, cap, page, magic, shift = dims
    n_chips = n_dev // 2
    o_dst = 3 * seq_dev + n_moves
    me = who_ref[0]
    base = me * n_slots

    @pl.loop(0, n_chips)
    def _(i):
        count[i] = 0

    @pl.loop(0, n_slots, unroll=8)
    def _(i):
        arrive_ref[i] = -1
        arrive_ref[n_slots + i] = -1

    @pl.loop(0, n_dev * cap, unroll=8)
    def _(i):
        pages_ref[i] = 0

    @pl.loop(0, n_dev)
    def _(d):
        for j in range(n_moves):
            dst = tab_ref[d, o_dst + j]
            m = d * n_moves + j
            dd = (dst * magic) >> shift
            chip = dd >> 1
            n = count[chip]
            count[chip] = n + 1

            @pl.when(n < 2 * cap)
            def _():
                pages_ref[chip * 2 * cap + n] = m

            @pl.when(dd == me)
            def _():
                arrive_ref[dst - base] = n
                arrive_ref[n_slots + dst - base] = m

    most_ref[0] = lax.fori_loop(0, n_chips, lambda i, best: jnp.maximum(best, count[i]), jnp.int32(0))


def cells_kernel(dims, who_ref, tab_ref, none_ref, info_ref, used_ref, moved, seen, sem):
    n_dev, n_cols, n_slots, seq_dev, n_moves, cap, page, magic, shift = dims
    o_len, o_src, o_dst = 2 * seq_dev, 3 * seq_dev, 3 * seq_dev + n_moves
    row0 = who_ref[1]
    base = who_ref[0] * n_slots
    fill = pltpu.make_async_copy(none_ref, moved, sem)
    fill.start()

    @pl.loop(0, n_cols * seq_dev, unroll=8)
    def _(i):
        seen[i] = 0

    @pl.loop(0, n_slots, unroll=8)
    def _(i):
        info_ref[i] = -1
        info_ref[n_slots + i] = -1

    fill.wait()

    @pl.loop(0, n_dev)
    def _(d):
        for j in range(n_moves):
            moved[tab_ref[d, o_src + j]] = tab_ref[d, o_dst + j]

    @pl.loop(0, n_cols)
    def _(h):
        @pl.loop(0, seq_dev, unroll=4)
        def _(i):
            b = h * seq_dev + i
            length = tab_ref[row0 + h, o_len + i]
            for j in range(2):
                e = tab_ref[row0 + h, 2 * i + j]
                e0 = jnp.maximum(e, 0)
                mv = moved[e0]
                s = jnp.where(mv >= 0, mv, e0) - base

                @pl.when((e >= 0) & (s >= 0) & (s < n_slots))
                def _():
                    info_ref[n_slots + s] = b
                    info_ref[2 * n_slots + s] = length - page * j

    def visit(s, n):
        b = info_ref[n_slots + s]

        @pl.when(b >= 0)
        def _():
            info_ref[n] = s
            info_ref[3 * n_slots + s] = seen[b]
            seen[b] = 1

        return n + jnp.where(b >= 0, 1, 0)

    used_ref[0] = lax.fori_loop(0, n_slots, visit, jnp.int32(0))


def pack_kernel(n_moves, src_ref, k_ref, v_ref, *rest):
    *outs, sem = rest

    def copies(m):
        s = src_ref[m]
        for layer, o_ref in enumerate(outs):
            half = o_ref.shape[0] // 2
            for a, pool in enumerate((k_ref, v_ref)):
                yield pltpu.make_async_copy(pool.at[s, layer], o_ref.at[pl.ds(a * half, half), m], sem.at[layer, a, m])

    for m in range(n_moves):
        for c in copies(m):
            c.start()
    for m in range(n_moves):
        for c in copies(m):
            c.wait()


def regroup_kernel(cap, pages_ref, x_ref, o_ref):
    @pl.loop(0, o_ref.shape[0])
    def _(d):
        for n in range(cap):
            o_ref[d, n] = x_ref[pages_ref[d * cap + n]]


def attend_kernel(dims, who_ref, arrive_ref, most_ref, info_ref, used_ref, q_ref, k_ref, v_ref, own_ref, mate_ref, slow_ref, *rest):
    layer, n_slots, cap, scale, quads, first = dims
    ko_ref, vo_ref, o_ref, ml_ref, kbuf, vbuf, in_sem, out_sem = rest if first else rest[2:]
    n_key, lanes = kbuf.shape[1] * kbuf.shape[2], kbuf.shape[3]
    n_ch = kbuf.shape[1]
    rows = o_ref.shape[1]
    over = most_ref[0] > 2 * cap
    core = who_ref[2]
    bufs = (kbuf, vbuf)
    part = pl.ds(layer * n_ch, n_ch)

    @pl.loop(0, n_slots)
    def _(s):
        n = arrive_ref[s]
        has = n >= 0
        half = jnp.where(n >= cap, 1, 0)
        pos = n - half * cap

        def go(cond, src_of):
            @pl.when(cond)
            def _():
                for a in range(2):
                    pltpu.make_async_copy(src_of(a), bufs[a].at[s], in_sem.at[a]).start()

        fast = has & jnp.logical_not(over)
        go(jnp.logical_not(has), lambda a: (k_ref, v_ref)[a].at[s, part])
        go(has & over, lambda a: slow_ref.at[layer, s, pl.ds(a * n_ch, n_ch)])
        go(fast & (half == core), lambda a: own_ref.at[pl.ds(a * n_ch, n_ch), pos])
        go(fast & (half != core), lambda a: mate_ref.at[pl.ds(a * n_ch, n_ch), pos])

    o_ref[...] = jnp.zeros_like(o_ref)
    ml_lane = lax.broadcasted_iota(jnp.int32, ml_ref.shape, 1)
    ml_ref[...] = jnp.where(ml_lane < rows, NEG, 0.0)
    for a in range(2):
        pltpu.make_async_copy((k_ref, v_ref)[a].at[:, part], bufs[a], in_sem.at[a]).wait()

    n_used = used_ref[0]
    tile = kbuf.shape[2]
    tile_row = lax.broadcasted_iota(jnp.int32, (tile, lanes), 0)

    @pl.loop(0, n_used)
    def _(i):
        s = info_ref[i]
        lim = info_ref[2 * n_slots + s]

        @pl.when(lim < n_key // 2)
        def _():
            fresh = q_ref[info_ref[n_slots + s], rows:].astype(F32)
            row0 = 2 * lim
            for c in (row0 // tile, jnp.minimum((row0 + 3) // tile, n_ch - 1)):
                at = tile_row + c * tile - row0
                for a, buf in enumerate(bufs):
                    x = buf[s, c].astype(F32)
                    for r in range(4):
                        x = jnp.where(at == r, fresh[4 * a + r:4 * a + r + 1], x)
                    buf[s, c] = x.astype(BF16)

    outs = [pltpu.make_async_copy(bufs[a], (ko_ref, vo_ref)[a].at[:, part], out_sem.at[a]) for a in range(2)]
    for c in outs:
        c.start()

    lane = lax.broadcasted_iota(jnp.int32, (rows, n_key), 1)
    row = lax.broadcasted_iota(jnp.int32, (rows, n_key), 0)
    own_head = (lane & 1) == ((row >> 3) & 1)
    late = (lane >> 1) - (row >> 4)
    out_lane = lax.broadcasted_iota(jnp.int32, (rows, lanes), 1)
    out_row = lax.broadcasted_iota(jnp.int32, (rows, lanes), 0)
    nothing = jnp.zeros((rows, n_key), BF16)

    @pl.loop(0, (n_used + 4 * quads - 1) // (4 * quads))
    def _(u):
        done = []
        for quad in range(quads):
            facts = []
            for t in range(4):
                i = (u * quads + quad) * 4 + t
                listed = info_ref[jnp.minimum(i, n_slots - 1)]
                used = (i < n_slots) & (listed >= 0)
                s = jnp.where(used, listed, 0)
                facts.append((s, used, jnp.maximum(info_ref[n_slots + s], 0), info_ref[2 * n_slots + s], info_ref[3 * n_slots + s]))
            q = jnp.concatenate([q_ref[f[2], :rows] for f in facts], axis=0)
            k = jnp.concatenate([kbuf[f[0]].reshape(n_key, lanes) for f in facts], axis=0)
            v = jnp.concatenate([vbuf[f[0]].reshape(n_key, lanes) for f in facts], axis=0)
            scores = lax.dot_general(q, k, (((1,), (1,)), ((), ())), preferred_element_type=F32)
            ps, stats = [], []
            for t, (s, used, b, lim, again) in enumerate(facts):
                sc = scores[t * rows:(t + 1) * rows, t * n_key:(t + 1) * n_key] * scale
                sc = jnp.where(own_head & (late <= lim), sc, NEG)
                m = jnp.max(sc, axis=1, keepdims=True)
                p = jnp.exp(sc - m)
                stats.append((m, jnp.sum(p, axis=1, keepdims=True)))
                ps.append(jnp.concatenate([p.astype(BF16) if x == t else nothing for x in range(4)], axis=1))
            o = jnp.dot(jnp.concatenate(ps, axis=0), v, preferred_element_type=F32)
            for t, (s, used, b, lim, again) in enumerate(facts):
                done.append((used, b, *stats[t], o[t * rows:(t + 1) * rows], again))
        for used, b0, m, l, o, again in done:
            def put(m, l, o):
                o_ref[b0] = o
                ml = jnp.where(out_lane == out_row, m, 0.0) + jnp.where(out_lane == out_row + rows, l, 0.0)
                ml_ref[pl.ds(b0, 1)] = jnp.sum(ml, axis=0, keepdims=True)

            @pl.when(used & (again == 0))
            def _():
                put(m, l, o)

            @pl.when(used & (again > 0))
            def _():
                old = jnp.broadcast_to(ml_ref[pl.ds(b0, 1)], (rows, lanes))
                m1 = jnp.sum(jnp.where(out_lane == out_row, old, 0.0), axis=1, keepdims=True)
                l1 = jnp.sum(jnp.where(out_lane == out_row + rows, old, 0.0), axis=1, keepdims=True)
                mm = jnp.maximum(m, m1)
                w, w1 = jnp.exp(m - mm), jnp.exp(m1 - mm)
                put(mm, l * w + l1 * w1, o * w + o_ref[b0] * w1)

    for c in outs:
        c.wait()


def blank_kernel(o_ref):
    pass


def sems(*shape):
    return pltpu.SemaphoreType.DMA(shape)


def comm(cid):
    return pltpu.CompilerParams(collective_id=cid, has_side_effects=True)


def solution(mesh):
    n_rows = mesh.shape['kv2']
    n_cols = mesh.shape['kv']
    n_dev = n_rows * n_cols
    dev_axes = ('rep', 'kv2', 'kv')
    seq_spec = P(None, dev_axes, None)
    pool_spec = P(dev_axes, None, None, None, None)
    table_spec = P(dev_axes, None)
    vec_spec = P(dev_axes)
    full_spec = P()

    def per_device(x_embed, w_query, w_key, w_value, w_out, w_up, w_down, k_pool, v_pool, old_table, seq_len, src_slot, dst_slot):
        n_slots, layers, page, kv_heads, head_dim = k_pool.shape
        heads = w_query.shape[2] // head_dim
        n_steps, seq_dev, width = x_embed.shape
        n_moves = src_slot.shape[0]
        row_seqs = seq_dev * n_cols
        rows = n_steps * heads
        key_rows = page * kv_heads
        tile = 8
        n_ch = key_rows // tile
        chunks = 2 * n_ch
        cap = 20
        assert chunks == n_dev and rows == 32 and old_table.shape[1] == 2
        shift = 18
        magic = -(-(1 << shift) // n_slots)
        assert all((s * magic) >> shift == s // n_slots for s in range(n_dev * n_slots))
        me = flat_id(n_cols)
        who = jnp.stack([me, lax.axis_index('kv2') * n_cols, lax.axis_index('kv') % 2]).astype(jnp.int32)

        kp = k_pool.reshape(n_slots, layers, n_ch, tile, head_dim)
        vp = v_pool.reshape(n_slots, layers, n_ch, tile, head_dim)
        kp4 = k_pool.reshape(n_slots, layers * n_ch, tile, head_dim)
        vp4 = v_pool.reshape(n_slots, layers * n_ch, tile, head_dim)
        packed = pl.pallas_call(
            functools.partial(pack_kernel, n_moves),
            out_shape=[jax.ShapeDtypeStruct((chunks, n_moves, tile, head_dim), BF16)] * layers,
            in_specs=[SMEM, ANY, ANY], out_specs=[VMEM] * layers,
            scratch_shapes=[sems(layers, 2, n_moves)], name='pack_pages')(src_slot - me * n_slots, kp, vp)
        after = lax.optimization_barrier

        mine = jnp.concatenate([old_table.reshape(-1), seq_len, src_slot, dst_slot])
        mine = jnp.pad(mine, (0, 128 - mine.shape[0])).reshape(1, 128)
        tab = pl.pallas_call(
            functools.partial(gather_all_kernel, n_dev, n_cols),
            out_shape=jax.ShapeDtypeStruct((n_dev, 1, 128), jnp.int32),
            in_specs=[VMEM], out_specs=VMEM,
            scratch_shapes=[pltpu.SemaphoreType.DMA, sems(n_dev), sems(n_dev)],
            compiler_params=comm(0), name='gather_tables')(mine)

        tab = tab.reshape(n_dev, 128)
        moving, tab = after((packed[0], tab))
        spread = lax.all_to_all(moving, ('kv2', 'kv'), 0, 0, tiled=True)
        dims = (n_dev, n_cols, n_slots, seq_dev, n_moves, cap, page, magic, shift)
        pages, arrive, most = pl.pallas_call(
            functools.partial(places_kernel, dims),
            out_shape=(jax.ShapeDtypeStruct((n_dev * cap,), jnp.int32), jax.ShapeDtypeStruct((2 * n_slots,), jnp.int32),
                       jax.ShapeDtypeStruct((1,), jnp.int32)),
            in_specs=[SMEM, SMEM], out_specs=(SMEM, SMEM, SMEM),
            scratch_shapes=[pltpu.SMEM((n_dev // 2,), jnp.int32)], name='places')(who, tab)

        def regroup(spread, name):
            return pl.pallas_call(
                functools.partial(regroup_kernel, cap),
                out_shape=jax.ShapeDtypeStruct((n_dev, cap, tile, head_dim), BF16),
                in_specs=[SMEM, VMEM], out_specs=VMEM, name=name)(pages, spread.reshape(n_dev * n_moves, tile, head_dim))

        def deliver(grouped):
            return lax.all_to_all(grouped, ('kv2', 'kv'), 0, 0, tiled=True)

        def to_mate(own):
            return lax.ppermute(own, 'kv', [(i, i ^ 1) for i in range(n_cols)])

        def all_pages():
            found = []
            for p in packed:
                everything = lax.all_gather(p.swapaxes(0, 1), ('kv2', 'kv'), tiled=True)
                found.append(everything[jnp.maximum(arrive[n_slots:], 0)])
            return jnp.stack(found)

        def no_pages():
            return pl.pallas_call(
                blank_kernel, out_shape=jax.ShapeDtypeStruct((layers, n_slots, chunks, tile, head_dim), BF16), out_specs=ANY,
                name='blank')()

        slow = lax.cond(most[0] > 2 * cap, all_pages, no_pages)

        hidden = x_embed.reshape(n_steps * seq_dev, width)
        k_out = v_out = None
        for layer in range(layers):
            query = jnp.dot(hidden, w_query[layer], preferred_element_type=F32).astype(BF16)
            k_new = jnp.dot(hidden, w_key[layer], preferred_element_type=F32).astype(BF16)
            v_new = jnp.dot(hidden, w_value[layer], preferred_element_type=F32).astype(BF16)

            def by_seq(x):
                return x.reshape(n_steps, seq_dev, -1, head_dim).swapaxes(0, 1).reshape(seq_dev, -1, head_dim)

            load = jnp.concatenate([by_seq(query), by_seq(k_new), by_seq(v_new)], axis=1)
            q_rows = load.shape[1]
            if layer == 0:
                spread, load, pages = after((spread, load, pages))
                grouped, load, tab = after((regroup(spread, 'regroup_pages_0'), load, tab))
                own = deliver(grouped)
                info, n_used = pl.pallas_call(
                    functools.partial(cells_kernel, dims),
                    out_shape=(jax.ShapeDtypeStruct((4 * n_slots,), jnp.int32), jax.ShapeDtypeStruct((1,), jnp.int32)),
                    in_specs=[SMEM, SMEM, ANY], out_specs=(SMEM, SMEM),
                    scratch_shapes=[pltpu.SMEM((n_dev * n_slots,), jnp.int32), pltpu.SMEM((row_seqs,), jnp.int32), pltpu.SemaphoreType.DMA],
                    name='cells')(who, tab, jnp.full((n_dev * n_slots,), -1, jnp.int32))
                pool_shape = jax.ShapeDtypeStruct(kp4.shape, BF16)
                load, info = after((load, info))
            else:
                own, load = after((own, load))
                mate = to_mate(own)
            n_chips = n_cols // 2
            q_row = pl.pallas_call(
                functools.partial(row_gather_kernel, n_cols),
                out_shape=jax.ShapeDtypeStruct((n_cols, seq_dev, q_rows, head_dim), BF16),
                in_specs=[VMEM], out_specs=VMEM,
                scratch_shapes=[pltpu.SemaphoreType.DMA, sems(n_chips), sems(n_chips), sems(n_chips), sems(n_chips)],
                compiler_params=comm(3 + layer), name=f'gather_queries_{layer}')(load)

            first = layer == 0
            if first:
                own, q_row = after((own, q_row))
                mate = to_mate(own)
            last = layer == layers - 1
            if not last:
                moving, q_row = after((packed[layer + 1], q_row))
                spread = lax.all_to_all(moving, ('kv2', 'kv'), 0, 0, tiled=True)
            carried = () if first else (k_out, v_out)
            k_out, v_out, part, ml = pl.pallas_call(
                functools.partial(attend_kernel, (layer, n_slots, cap, head_dim ** -0.5, 2, first)),
                in_specs=[SMEM] * 5 + [VMEM] + [ANY] * (5 + len(carried)),
                out_specs=[ANY, ANY, VMEM, VMEM],
                out_shape=[pool_shape, pool_shape, jax.ShapeDtypeStruct((row_seqs, rows, head_dim), F32),
                           jax.ShapeDtypeStruct((row_seqs, head_dim), F32)],
                scratch_shapes=[pltpu.VMEM((n_slots, n_ch, tile, head_dim), BF16), pltpu.VMEM((n_slots, n_ch, tile, head_dim), BF16),
                                sems(2), sems(2)],
                input_output_aliases={} if first else {11: 0, 12: 1},
                name=f'attend_{layer}')(who, arrive, most, info, n_used, q_row.reshape(row_seqs, q_rows, head_dim), kp4, vp4,
                                        own, mate, slow, *carried)

            parts, parts_ml = (n_chips, seq_dev, rows, head_dim), (n_chips, seq_dev, head_dim)
            attn = pl.pallas_call(
                functools.partial(return_kernel, n_cols),
                out_shape=jax.ShapeDtypeStruct((n_steps, seq_dev, heads, head_dim), BF16),
                in_specs=[VMEM, VMEM], out_specs=VMEM,
                scratch_shapes=[pltpu.VMEM(shape, F32) for _ in range(3) for shape in (parts, parts_ml)] + [sems(2, n_chips)] * 4,
                compiler_params=comm(5 + layer), name=f'return_{layer}')(
                    part.reshape(n_cols, seq_dev, rows, head_dim), ml.reshape(n_cols, seq_dev, head_dim))
            attn_out = attn.reshape(n_steps * seq_dev, heads * head_dim)
            hidden = (hidden.astype(F32) + jnp.dot(attn_out, w_out[layer], preferred_element_type=F32)).astype(BF16)
            if not last:
                spread, hidden = after((spread, hidden))
                grouped, hidden = after((regroup(spread, f'regroup_pages_{layer + 1}'), hidden))
                own = deliver(grouped)
            up_act = jax.nn.gelu(jnp.dot(hidden, w_up[layer], preferred_element_type=F32)).astype(BF16)
            hidden = (hidden.astype(F32) + jnp.dot(up_act, w_down[layer], preferred_element_type=F32)).astype(BF16)
        return hidden.reshape(x_embed.shape), k_out.reshape(k_pool.shape), v_out.reshape(v_pool.shape)

    return jax.shard_map(per_device, mesh=mesh, in_specs=(seq_spec, full_spec, full_spec, full_spec, full_spec, full_spec, full_spec, pool_spec, pool_spec, table_spec, vec_spec, vec_spec, vec_spec), out_specs=(seq_spec, pool_spec, pool_spec), check_vma=False)
```

```python
import functools

import jax
import jax.numpy as jnp
from jax import lax
from jax.experimental import pallas as pl
from jax.experimental.pallas import tpu as pltpu
from jax.sharding import PartitionSpec as P

MESH = pl.DeviceIdType.MESH
ANY = pl.BlockSpec(memory_space=pl.ANY)
SMEM = pl.BlockSpec(memory_space=pltpu.SMEM)
VMEM = pl.BlockSpec(memory_space=pltpu.VMEM)
F32 = jnp.float32
BF16 = jnp.bfloat16
NEG = -1e30


def flat_id(n_cols):
    return lax.axis_index('kv2') * n_cols + lax.axis_index('kv')


def where_is(flat, n_cols):
    return {'kv2': flat // n_cols, 'kv': flat % n_cols}


def greet_all(n_dev, n_cols):
    me = flat_id(n_cols)
    barrier = pltpu.get_barrier_semaphore()

    @pl.loop(1, n_dev)
    def _(r):
        pl.semaphore_signal(barrier, inc=1, device_id=where_is((me + r) % n_dev, n_cols), device_id_type=MESH)

    pl.semaphore_wait(barrier, n_dev - 1)


def gather_all_kernel(n_dev, n_cols, x_ref, o_ref, local_sem, send_sem, recv_sem):
    me = flat_id(n_cols)
    greet_all(n_dev, n_cols)

    def copy(r, dst, slot):
        return pltpu.make_async_remote_copy(
            src_ref=x_ref, dst_ref=o_ref.at[slot], send_sem=send_sem.at[r], recv_sem=recv_sem.at[r],
            device_id=where_is(dst, n_cols), device_id_type=MESH)

    @pl.loop(1, n_dev)
    def _(r):
        copy(r, (me + r) % n_dev, me).start()

    own = pltpu.make_async_copy(x_ref, o_ref.at[me], local_sem)
    own.start()
    own.wait()

    @pl.loop(1, n_dev)
    def _(r):
        c = copy(r, (me + r) % n_dev, (me + n_dev - r) % n_dev)
        c.wait_send()
        c.wait_recv()


def row_gather_kernel(n_cols, x_ref, o_ref, local_sem, send_sem, recv_sem, fsend_sem, frecv_sem):
    n_chips = n_cols // 2
    kv = lax.axis_index('kv')
    chip, core = kv // 2, kv % 2
    mate = chip * 2 + 1 - core
    barrier = pltpu.get_barrier_semaphore()
    for r in range(1, n_chips):
        pl.semaphore_signal(barrier, inc=1, device_id={'kv': (chip + r) % n_chips * 2 + core}, device_id_type=MESH)
    pl.semaphore_signal(barrier, inc=1, device_id={'kv': mate}, device_id_type=MESH)
    pl.semaphore_wait(barrier, n_chips)

    def copy(r, dst, slot):
        return pltpu.make_async_remote_copy(
            src_ref=x_ref, dst_ref=o_ref.at[slot], send_sem=send_sem.at[r], recv_sem=recv_sem.at[r],
            device_id={'kv': dst}, device_id_type=MESH)

    def forward(r, slot):
        return pltpu.make_async_remote_copy(
            src_ref=o_ref.at[slot], dst_ref=o_ref.at[slot], send_sem=fsend_sem.at[r], recv_sem=frecv_sem.at[r],
            device_id={'kv': mate}, device_id_type=MESH)

    for r in range(1, n_chips):
        copy(r, (chip + r) % n_chips * 2 + core, kv).start()
    copy(0, mate, kv).start()
    own = pltpu.make_async_copy(x_ref, o_ref.at[kv], local_sem)
    own.start()
    own.wait()
    for r in range(1, n_chips):
        slot = (chip + n_chips - r) % n_chips * 2 + core
        copy(r, mate, slot).wait_recv()
        forward(r, slot).start()
    for r in range(1, n_chips):
        copy(r, mate, kv).wait_send()
        forward(r, (chip + n_chips - r) % n_chips * 2 + core).wait_send()
        forward(r, (chip + n_chips - r) % n_chips * 2 + 1 - core).wait_recv()
    c = copy(0, mate, mate)
    c.wait_send()
    c.wait_recv()


def return_kernel(n_cols, x_ref, ml_ref, out_ref, mate_o, mate_ml, sum_o, sum_ml, got_o, got_ml, dsend, drecv, send, recv):
    n_chips = n_cols // 2
    kv = lax.axis_index('kv')
    chip, core = kv // 2, kv % 2
    mate = chip * 2 + 1 - core
    seq_dev, rows, lanes = x_ref.shape[1:]
    heads = out_ref.shape[2]
    barrier = pltpu.get_barrier_semaphore()
    for r in range(1, n_chips):
        pl.semaphore_signal(barrier, inc=1, device_id={'kv': (chip + r) % n_chips * 2 + core}, device_id_type=MESH)
    pl.semaphore_signal(barrier, inc=1, device_id={'kv': mate}, device_id_type=MESH)
    pl.semaphore_wait(barrier, n_chips)

    def across(r, a):
        src, dst = ((x_ref, mate_o), (ml_ref, mate_ml))[a]
        return pltpu.make_async_remote_copy(
            src_ref=src.at[(chip + r) % n_chips * 2 + 1 - core], dst_ref=dst.at[r], send_sem=dsend.at[a, r], recv_sem=drecv.at[a, r],
            device_id={'kv': mate}, device_id_type=MESH)

    def home(r, a):
        src, dst = ((sum_o, got_o), (sum_ml, got_ml))[a]
        return pltpu.make_async_remote_copy(
            src_ref=src.at[r], dst_ref=dst.at[r], send_sem=send.at[a, r], recv_sem=recv.at[a, r],
            device_id={'kv': (chip + r) % n_chips * 2 + core}, device_id_type=MESH)

    order = sorted(range(1, n_chips), key=lambda r: -min(r, n_chips - r)) + [0]
    for r in order:
        for a in range(2):
            across(r, a).start()
    lane = lax.broadcasted_iota(jnp.int32, (8, lanes), 1)
    for r in order:
        slot = (chip + r) % n_chips * 2 + core
        to_o, to_ml = (sum_o, sum_ml) if r else (got_o, got_ml)
        for a in range(2):
            across(r, a).wait_recv()

        @pl.loop(0, seq_dev // 8)
        def _(g):
            some = pl.ds(pl.multiple_of(8 * g, 8), 8)
            ml1, ml2 = ml_ref[slot, some], mate_ml[r, some]
            top = jnp.maximum(ml1, ml2)
            w1, w2 = jnp.exp(ml1 - top), jnp.exp(ml2 - top)
            l = pltpu.roll(w1, rows, 1) * ml1 + pltpu.roll(w2, rows, 1) * ml2
            to_ml[r, some] = jnp.where(lane < rows, top, l)
            c1, c2 = w1.T, w2.T
            for t in range(8):
                b = 8 * g + t
                to_o[r, b] = c1[:rows, t:t + 1] * x_ref[slot, b] + c2[:rows, t:t + 1] * mate_o[r, b]

        if r:
            for a in range(2):
                home(r, a).start()
    for r in range(1, n_chips):
        for a in range(2):
            home(r, a).wait_recv()

    @pl.loop(0, seq_dev // 8)
    def _(g):
        some = pl.ds(pl.multiple_of(8 * g, 8), 8)
        mls = [got_ml[p, some] for p in range(n_chips)]
        top = functools.reduce(jnp.maximum, mls)
        ws = [jnp.exp(x - top) for x in mls]
        total = sum(w * pltpu.roll(x, lanes - rows, 1) for w, x in zip(ws, mls))
        cols = [(w / total).T for w in ws]
        for t in range(8):
            b = 8 * g + t
            acc = sum(c[:rows, t:t + 1] * got_o[p, b] for p, c in enumerate(cols)).astype(BF16)
            out_ref[0, b] = acc[:heads]
            out_ref[1, b] = acc[heads:]

    for r in range(n_chips):
        for a in range(2):
            across(r, a).wait_send()
            if r:
                home(r, a).wait_send()


def places_kernel(dims, who_ref, tab_ref, pages_ref, arrive_ref, most_ref, count):
    n_dev, n_cols, n_slots, seq_dev, n_moves, cap, page, magic, shift = dims
    n_chips = n_dev // 2
    o_dst = 3 * seq_dev + n_moves
    me = who_ref[0]
    base = me * n_slots

    @pl.loop(0, n_chips)
    def _(i):
        count[i] = 0

    @pl.loop(0, n_slots, unroll=8)
    def _(i):
        arrive_ref[i] = -1
        arrive_ref[n_slots + i] = -1

    @pl.loop(0, n_dev * cap, unroll=8)
    def _(i):
        pages_ref[i] = 0

    @pl.loop(0, n_dev)
    def _(d):
        for j in range(n_moves):
            dst = tab_ref[d, o_dst + j]
            m = d * n_moves + j
            dd = (dst * magic) >> shift
            chip = dd >> 1
            n = count[chip]
            count[chip] = n + 1

            @pl.when(n < 2 * cap)
            def _():
                pages_ref[chip * 2 * cap + n] = m

            @pl.when(dd == me)
            def _():
                arrive_ref[dst - base] = n
                arrive_ref[n_slots + dst - base] = m

    most_ref[0] = lax.fori_loop(0, n_chips, lambda i, best: jnp.maximum(best, count[i]), jnp.int32(0))


def cells_kernel(dims, who_ref, tab_ref, none_ref, info_ref, used_ref, moved, seen, sem):
    n_dev, n_cols, n_slots, seq_dev, n_moves, cap, page, magic, shift = dims
    o_len, o_src, o_dst = 2 * seq_dev, 3 * seq_dev, 3 * seq_dev + n_moves
    row0 = who_ref[1]
    base = who_ref[0] * n_slots
    fill = pltpu.make_async_copy(none_ref, moved, sem)
    fill.start()

    @pl.loop(0, n_cols * seq_dev, unroll=8)
    def _(i):
        seen[i] = 0

    @pl.loop(0, n_slots, unroll=8)
    def _(i):
        info_ref[i] = -1
        info_ref[n_slots + i] = -1

    fill.wait()

    @pl.loop(0, n_dev)
    def _(d):
        for j in range(n_moves):
            moved[tab_ref[d, o_src + j]] = tab_ref[d, o_dst + j]

    @pl.loop(0, n_cols)
    def _(h):
        @pl.loop(0, seq_dev, unroll=4)
        def _(i):
            b = h * seq_dev + i
            length = tab_ref[row0 + h, o_len + i]
            for j in range(2):
                e = tab_ref[row0 + h, 2 * i + j]
                e0 = jnp.maximum(e, 0)
                mv = moved[e0]
                s = jnp.where(mv >= 0, mv, e0) - base

                @pl.when((e >= 0) & (s >= 0) & (s < n_slots))
                def _():
                    info_ref[n_slots + s] = b
                    info_ref[2 * n_slots + s] = length - page * j

    def visit(s, n):
        b = info_ref[n_slots + s]

        @pl.when(b >= 0)
        def _():
            info_ref[n] = s
            info_ref[3 * n_slots + s] = seen[b]
            seen[b] = 1

        return n + jnp.where(b >= 0, 1, 0)

    used_ref[0] = lax.fori_loop(0, n_slots, visit, jnp.int32(0))


def pack_kernel(n_moves, src_ref, k_ref, v_ref, *rest):
    *outs, sem = rest

    def copies(m):
        s = src_ref[m]
        for layer, o_ref in enumerate(outs):
            half = o_ref.shape[0] // 2
            for a, pool in enumerate((k_ref, v_ref)):
                yield pltpu.make_async_copy(pool.at[s, layer], o_ref.at[pl.ds(a * half, half), m], sem.at[layer, a, m])

    for m in range(n_moves):
        for c in copies(m):
            c.start()
    for m in range(n_moves):
        for c in copies(m):
            c.wait()


def regroup_kernel(cap, pages_ref, x_ref, o_ref):
    @pl.loop(0, o_ref.shape[0])
    def _(d):
        for n in range(cap):
            o_ref[d, n] = x_ref[pages_ref[d * cap + n]]


def attend_kernel(dims, who_ref, arrive_ref, most_ref, info_ref, used_ref, q_ref, k_ref, v_ref, own_ref, mate_ref, slow_ref, *rest):
    layer, n_slots, cap, scale, quads, first = dims
    ko_ref, vo_ref, o_ref, ml_ref, kbuf, vbuf, in_sem, out_sem = rest if first else rest[2:]
    n_key, lanes = kbuf.shape[1] * kbuf.shape[2], kbuf.shape[3]
    n_ch = kbuf.shape[1]
    rows = o_ref.shape[1]
    over = most_ref[0] > 2 * cap
    core = who_ref[2]
    bufs = (kbuf, vbuf)
    part = pl.ds(layer * n_ch, n_ch)

    @pl.loop(0, n_slots)
    def _(s):
        n = arrive_ref[s]
        has = n >= 0
        half = jnp.where(n >= cap, 1, 0)
        pos = n - half * cap

        def go(cond, src_of):
            @pl.when(cond)
            def _():
                for a in range(2):
                    pltpu.make_async_copy(src_of(a), bufs[a].at[s], in_sem.at[a]).start()

        fast = has & jnp.logical_not(over)
        go(jnp.logical_not(has), lambda a: (k_ref, v_ref)[a].at[s, part])
        go(has & over, lambda a: slow_ref.at[layer, s, pl.ds(a * n_ch, n_ch)])
        go(fast & (half == core), lambda a: own_ref.at[pl.ds(a * n_ch, n_ch), pos])
        go(fast & (half != core), lambda a: mate_ref.at[pl.ds(a * n_ch, n_ch), pos])

    o_ref[...] = jnp.zeros_like(o_ref)
    ml_lane = lax.broadcasted_iota(jnp.int32, ml_ref.shape, 1)
    ml_ref[...] = jnp.where(ml_lane < rows, NEG, 0.0)
    for a in range(2):
        pltpu.make_async_copy((k_ref, v_ref)[a].at[:, part], bufs[a], in_sem.at[a]).wait()

    n_used = used_ref[0]
    tile = kbuf.shape[2]
    tile_row = lax.broadcasted_iota(jnp.int32, (tile, lanes), 0)

    @pl.loop(0, n_used)
    def _(i):
        s = info_ref[i]
        lim = info_ref[2 * n_slots + s]

        @pl.when(lim < n_key // 2)
        def _():
            fresh = q_ref[info_ref[n_slots + s], rows:].astype(F32)
            row0 = 2 * lim
            for c in (row0 // tile, jnp.minimum((row0 + 3) // tile, n_ch - 1)):
                at = tile_row + c * tile - row0
                for a, buf in enumerate(bufs):
                    x = buf[s, c].astype(F32)
                    for r in range(4):
                        x = jnp.where(at == r, fresh[4 * a + r:4 * a + r + 1], x)
                    buf[s, c] = x.astype(BF16)

    outs = [pltpu.make_async_copy(bufs[a], (ko_ref, vo_ref)[a].at[:, part], out_sem.at[a]) for a in range(2)]
    for c in outs:
        c.start()

    lane = lax.broadcasted_iota(jnp.int32, (rows, n_key), 1)
    row = lax.broadcasted_iota(jnp.int32, (rows, n_key), 0)
    own_head = (lane & 1) == ((row >> 3) & 1)
    late = (lane >> 1) - (row >> 4)
    out_lane = lax.broadcasted_iota(jnp.int32, (rows, lanes), 1)
    out_row = lax.broadcasted_iota(jnp.int32, (rows, lanes), 0)
    nothing = jnp.zeros((rows, n_key), BF16)

    @pl.loop(0, (n_used + 4 * quads - 1) // (4 * quads))
    def _(u):
        done = []
        for quad in range(quads):
            facts = []
            for t in range(4):
                i = (u * quads + quad) * 4 + t
                listed = info_ref[jnp.minimum(i, n_slots - 1)]
                used = (i < n_slots) & (listed >= 0)
                s = jnp.where(used, listed, 0)
                facts.append((s, used, jnp.maximum(info_ref[n_slots + s], 0), info_ref[2 * n_slots + s], info_ref[3 * n_slots + s]))
            q = jnp.concatenate([q_ref[f[2], :rows] for f in facts], axis=0)
            k = jnp.concatenate([kbuf[f[0]].reshape(n_key, lanes) for f in facts], axis=0)
            v = jnp.concatenate([vbuf[f[0]].reshape(n_key, lanes) for f in facts], axis=0)
            scores = lax.dot_general(q, k, (((1,), (1,)), ((), ())), preferred_element_type=F32)
            ps, stats = [], []
            for t, (s, used, b, lim, again) in enumerate(facts):
                sc = scores[t * rows:(t + 1) * rows, t * n_key:(t + 1) * n_key] * scale
                sc = jnp.where(own_head & (late <= lim), sc, NEG)
                m = jnp.max(sc, axis=1, keepdims=True)
                p = jnp.exp(sc - m)
                stats.append((m, jnp.sum(p, axis=1, keepdims=True)))
                ps.append(jnp.concatenate([p.astype(BF16) if x == t else nothing for x in range(4)], axis=1))
            o = jnp.dot(jnp.concatenate(ps, axis=0), v, preferred_element_type=F32)
            for t, (s, used, b, lim, again) in enumerate(facts):
                done.append((used, b, *stats[t], o[t * rows:(t + 1) * rows], again))
        for used, b0, m, l, o, again in done:
            def put(m, l, o):
                o_ref[b0] = o
                ml = jnp.where(out_lane == out_row, m, 0.0) + jnp.where(out_lane == out_row + rows, l, 0.0)
                ml_ref[pl.ds(b0, 1)] = jnp.sum(ml, axis=0, keepdims=True)

            @pl.when(used & (again == 0))
            def _():
                put(m, l, o)

            @pl.when(used & (again > 0))
            def _():
                old = jnp.broadcast_to(ml_ref[pl.ds(b0, 1)], (rows, lanes))
                m1 = jnp.sum(jnp.where(out_lane == out_row, old, 0.0), axis=1, keepdims=True)
                l1 = jnp.sum(jnp.where(out_lane == out_row + rows, old, 0.0), axis=1, keepdims=True)
                mm = jnp.maximum(m, m1)
                w, w1 = jnp.exp(m - mm), jnp.exp(m1 - mm)
                put(mm, l * w + l1 * w1, o * w + o_ref[b0] * w1)

    for c in outs:
        c.wait()


def mlp_kernel(layer, depth, attn_ref, hid_ref, wo_ref, up_ref, dn_ref, out_ref, abuf, bbuf, x_all, u, acc, got, a_sem, b_sem, send, recv):
    kv = lax.axis_index('kv')
    core = kv % 2
    mate = kv + 1 - 2 * core
    width, tile = abuf.shape[1:]
    n_out = width // tile
    n_up = -(-up_ref.shape[2] // (2 * tile))
    base = core * (up_ref.shape[2] - n_up * tile)
    both = 2 * n_up * tile - up_ref.shape[2]
    chunk = 256

    def cols(t):
        return pl.ds(pl.multiple_of(base + t * tile, chunk), tile)

    def load_out(n):
        return pltpu.make_async_copy(wo_ref.at[layer, :, pl.ds(n * tile, tile)], abuf.at[n % depth], a_sem.at[n % depth])

    def load_up(t):
        slot = (t + n_out) % depth
        return pltpu.make_async_copy(up_ref.at[layer, :, cols(t)], abuf.at[slot], a_sem.at[slot])

    def load_down(t):
        slot = t % depth
        return pltpu.make_async_copy(dn_ref.at[layer, cols(t), :], bbuf.at[slot], b_sem.at[slot])

    for n in range(min(depth, n_out)):
        load_out(n).start()
    for t in range(depth):
        load_down(t).start()
    barrier = pltpu.get_barrier_semaphore()
    pl.semaphore_signal(barrier, inc=1, device_id={'kv': mate}, device_id_type=MESH)
    pl.semaphore_wait(barrier, 1)

    def across(src, dst, i):
        return pltpu.make_async_remote_copy(
            src_ref=src, dst_ref=dst, send_sem=send.at[i], recv_sem=recv.at[i], device_id={'kv': mate}, device_id_type=MESH)

    for n in range(n_out):
        load_out(n).wait()
        part = slice(n * tile, (n + 1) * tile)
        y = jnp.dot(attn_ref[...], abuf[n % depth], preferred_element_type=F32)
        x_all[core, :, part] = (hid_ref[:, part].astype(F32) + y).astype(BF16)
        later = n + depth
        if later < n_out:
            load_out(later).start()
        else:
            load_up(later - n_out).start()
    share = across(x_all.at[core], x_all.at[core], 0)
    share.start()
    acc[...] = jnp.zeros_like(acc)
    share.wait_send()
    across(x_all.at[core], x_all.at[1 - core], 0).wait_recv()

    @pl.loop(0, n_up)
    def _(t):
        slot = (t + n_out) % depth
        load_up(t).wait()
        x = x_all[...].reshape(-1, width)
        for c in range(tile // chunk):
            part = slice(c * chunk, (c + 1) * chunk)
            y = jax.nn.gelu(jnp.dot(x, abuf[slot, :, part], preferred_element_type=F32)).astype(BF16)
            if c * chunk < both:
                y = jnp.where((core == 1) & (t == 0), jnp.zeros_like(y), y)
            u[:, part] = y

        @pl.when(t + depth < n_up)
        def _():
            load_up(t + depth).start()

        load_down(t).wait()
        for c in range(width // tile):
            part = slice(c * tile, (c + 1) * tile)
            y = jnp.dot(u[...], bbuf[t % depth, :, part], preferred_element_type=F32)
            acc[:, :, part] += y.reshape(acc.shape[0], acc.shape[1], tile)

        @pl.when(t + depth < n_up)
        def _():
            load_down(t + depth).start()

    give = across(acc.at[1 - core], got, 1)
    give.start()
    give.wait()
    out_ref[...] = (x_all[core].astype(F32) + (acc[core] + got[...])).astype(BF16)


def blank_kernel(o_ref):
    pass


def sems(*shape):
    return pltpu.SemaphoreType.DMA(shape)


def comm(cid):
    return pltpu.CompilerParams(collective_id=cid, has_side_effects=True)


def solution(mesh):
    n_rows = mesh.shape['kv2']
    n_cols = mesh.shape['kv']
    n_dev = n_rows * n_cols
    dev_axes = ('rep', 'kv2', 'kv')
    seq_spec = P(None, dev_axes, None)
    pool_spec = P(dev_axes, None, None, None, None)
    table_spec = P(dev_axes, None)
    vec_spec = P(dev_axes)
    full_spec = P()

    def per_device(x_embed, w_query, w_key, w_value, w_out, w_up, w_down, k_pool, v_pool, old_table, seq_len, src_slot, dst_slot):
        n_slots, layers, page, kv_heads, head_dim = k_pool.shape
        heads = w_query.shape[2] // head_dim
        n_steps, seq_dev, width = x_embed.shape
        n_moves = src_slot.shape[0]
        row_seqs = seq_dev * n_cols
        rows = n_steps * heads
        key_rows = page * kv_heads
        tile = 8
        n_ch = key_rows // tile
        chunks = 2 * n_ch
        cap = 20
        assert chunks == n_dev and rows == 32 and old_table.shape[1] == 2
        shift = 18
        magic = -(-(1 << shift) // n_slots)
        assert all((s * magic) >> shift == s // n_slots for s in range(n_dev * n_slots))
        me = flat_id(n_cols)
        who = jnp.stack([me, lax.axis_index('kv2') * n_cols, lax.axis_index('kv') % 2]).astype(jnp.int32)

        kp = k_pool.reshape(n_slots, layers, n_ch, tile, head_dim)
        vp = v_pool.reshape(n_slots, layers, n_ch, tile, head_dim)
        kp4 = k_pool.reshape(n_slots, layers * n_ch, tile, head_dim)
        vp4 = v_pool.reshape(n_slots, layers * n_ch, tile, head_dim)
        packed = pl.pallas_call(
            functools.partial(pack_kernel, n_moves),
            out_shape=[jax.ShapeDtypeStruct((chunks, n_moves, tile, head_dim), BF16)] * layers,
            in_specs=[SMEM, ANY, ANY], out_specs=[VMEM] * layers,
            scratch_shapes=[sems(layers, 2, n_moves)], name='pack_pages')(src_slot - me * n_slots, kp, vp)
        after = lax.optimization_barrier

        mine = jnp.concatenate([old_table.reshape(-1), seq_len, src_slot, dst_slot])
        mine = jnp.pad(mine, (0, 128 - mine.shape[0])).reshape(1, 128)
        tab = pl.pallas_call(
            functools.partial(gather_all_kernel, n_dev, n_cols),
            out_shape=jax.ShapeDtypeStruct((n_dev, 1, 128), jnp.int32),
            in_specs=[VMEM], out_specs=VMEM,
            scratch_shapes=[pltpu.SemaphoreType.DMA, sems(n_dev), sems(n_dev)],
            compiler_params=comm(0), name='gather_tables')(mine)

        tab = tab.reshape(n_dev, 128)
        moving, tab = after((packed[0], tab))
        spread = lax.all_to_all(moving, ('kv2', 'kv'), 0, 0, tiled=True)
        dims = (n_dev, n_cols, n_slots, seq_dev, n_moves, cap, page, magic, shift)
        pages, arrive, most = pl.pallas_call(
            functools.partial(places_kernel, dims),
            out_shape=(jax.ShapeDtypeStruct((n_dev * cap,), jnp.int32), jax.ShapeDtypeStruct((2 * n_slots,), jnp.int32),
                       jax.ShapeDtypeStruct((1,), jnp.int32)),
            in_specs=[SMEM, SMEM], out_specs=(SMEM, SMEM, SMEM),
            scratch_shapes=[pltpu.SMEM((n_dev // 2,), jnp.int32)], name='places')(who, tab)

        def regroup(spread, name):
            return pl.pallas_call(
                functools.partial(regroup_kernel, cap),
                out_shape=jax.ShapeDtypeStruct((n_dev, cap, tile, head_dim), BF16),
                in_specs=[SMEM, VMEM], out_specs=VMEM, name=name)(pages, spread.reshape(n_dev * n_moves, tile, head_dim))

        def deliver(grouped):
            return lax.all_to_all(grouped, ('kv2', 'kv'), 0, 0, tiled=True)

        def to_mate(own):
            return lax.ppermute(own, 'kv', [(i, i ^ 1) for i in range(n_cols)])

        def all_pages():
            found = []
            for p in packed:
                everything = lax.all_gather(p.swapaxes(0, 1), ('kv2', 'kv'), tiled=True)
                found.append(everything[jnp.maximum(arrive[n_slots:], 0)])
            return jnp.stack(found)

        def no_pages():
            return pl.pallas_call(
                blank_kernel, out_shape=jax.ShapeDtypeStruct((layers, n_slots, chunks, tile, head_dim), BF16), out_specs=ANY,
                name='blank')()

        slow = lax.cond(most[0] > 2 * cap, all_pages, no_pages)

        hidden = x_embed.reshape(n_steps * seq_dev, width)
        k_out = v_out = None
        for layer in range(layers):
            query = jnp.dot(hidden, w_query[layer], preferred_element_type=F32).astype(BF16)
            k_new = jnp.dot(hidden, w_key[layer], preferred_element_type=F32).astype(BF16)
            v_new = jnp.dot(hidden, w_value[layer], preferred_element_type=F32).astype(BF16)

            def by_seq(x):
                return x.reshape(n_steps, seq_dev, -1, head_dim).swapaxes(0, 1).reshape(seq_dev, -1, head_dim)

            load = jnp.concatenate([by_seq(query), by_seq(k_new), by_seq(v_new)], axis=1)
            q_rows = load.shape[1]
            if layer == 0:
                spread, load, pages = after((spread, load, pages))
                grouped, load, tab = after((regroup(spread, 'regroup_pages_0'), load, tab))
                own = deliver(grouped)
                info, n_used = pl.pallas_call(
                    functools.partial(cells_kernel, dims),
                    out_shape=(jax.ShapeDtypeStruct((4 * n_slots,), jnp.int32), jax.ShapeDtypeStruct((1,), jnp.int32)),
                    in_specs=[SMEM, SMEM, ANY], out_specs=(SMEM, SMEM),
                    scratch_shapes=[pltpu.SMEM((n_dev * n_slots,), jnp.int32), pltpu.SMEM((row_seqs,), jnp.int32), pltpu.SemaphoreType.DMA],
                    name='cells')(who, tab, jnp.full((n_dev * n_slots,), -1, jnp.int32))
                pool_shape = jax.ShapeDtypeStruct(kp4.shape, BF16)
                load, info = after((load, info))
            else:
                own, load = after((own, load))
                mate = to_mate(own)
            n_chips = n_cols // 2
            q_row = pl.pallas_call(
                functools.partial(row_gather_kernel, n_cols),
                out_shape=jax.ShapeDtypeStruct((n_cols, seq_dev, q_rows, head_dim), BF16),
                in_specs=[VMEM], out_specs=VMEM,
                scratch_shapes=[pltpu.SemaphoreType.DMA, sems(n_chips), sems(n_chips), sems(n_chips), sems(n_chips)],
                compiler_params=comm(3 + layer), name=f'gather_queries_{layer}')(load)

            first = layer == 0
            if first:
                own, q_row = after((own, q_row))
                mate = to_mate(own)
            last = layer == layers - 1
            if not last:
                moving, q_row = after((packed[layer + 1], q_row))
                spread = lax.all_to_all(moving, ('kv2', 'kv'), 0, 0, tiled=True)
            carried = () if first else (k_out, v_out)
            k_out, v_out, part, ml = pl.pallas_call(
                functools.partial(attend_kernel, (layer, n_slots, cap, head_dim ** -0.5, 2, first)),
                in_specs=[SMEM] * 5 + [VMEM] + [ANY] * (5 + len(carried)),
                out_specs=[ANY, ANY, VMEM, VMEM],
                out_shape=[pool_shape, pool_shape, jax.ShapeDtypeStruct((row_seqs, rows, head_dim), F32),
                           jax.ShapeDtypeStruct((row_seqs, head_dim), F32)],
                scratch_shapes=[pltpu.VMEM((n_slots, n_ch, tile, head_dim), BF16), pltpu.VMEM((n_slots, n_ch, tile, head_dim), BF16),
                                sems(2), sems(2)],
                input_output_aliases={} if first else {11: 0, 12: 1},
                name=f'attend_{layer}')(who, arrive, most, info, n_used, q_row.reshape(row_seqs, q_rows, head_dim), kp4, vp4,
                                        own, mate, slow, *carried)

            parts, parts_ml = (n_chips, seq_dev, rows, head_dim), (n_chips, seq_dev, head_dim)
            attn = pl.pallas_call(
                functools.partial(return_kernel, n_cols),
                out_shape=jax.ShapeDtypeStruct((n_steps, seq_dev, heads, head_dim), BF16),
                in_specs=[VMEM, VMEM], out_specs=VMEM,
                scratch_shapes=[pltpu.VMEM(shape, F32) for _ in range(3) for shape in (parts, parts_ml)] + [sems(2, n_chips)] * 4,
                compiler_params=comm(5 + layer), name=f'return_{layer}')(
                    part.reshape(n_cols, seq_dev, rows, head_dim), ml.reshape(n_cols, seq_dev, head_dim))
            attn_out = attn.reshape(n_steps * seq_dev, heads * head_dim)
            n_tok = n_steps * seq_dev
            if not last:
                spread, attn_out = after((spread, attn_out))
                grouped, attn_out = after((regroup(spread, f'regroup_pages_{layer + 1}'), attn_out))
                own = deliver(grouped)
            depth, wide = 4, 512
            assert w_up.shape[2] % 256 == 0 and width % wide == 0
            hidden = pl.pallas_call(
                functools.partial(mlp_kernel, layer, depth),
                out_shape=jax.ShapeDtypeStruct((n_tok, width), BF16),
                in_specs=[VMEM, VMEM, ANY, ANY, ANY], out_specs=VMEM,
                scratch_shapes=[pltpu.VMEM((depth, width, wide), BF16), pltpu.VMEM((depth, wide, width), BF16),
                                pltpu.VMEM((2, n_tok, width), BF16), pltpu.VMEM((2 * n_tok, wide), BF16),
                                pltpu.VMEM((2, n_tok, width), F32), pltpu.VMEM((n_tok, width), F32),
                                sems(depth), sems(depth), sems(2), sems(2)],
                compiler_params=comm(7 + layer), name=f'mlp_{layer}')(attn_out, hidden, w_out, w_up, w_down)
        return hidden.reshape(x_embed.shape), k_out.reshape(k_pool.shape), v_out.reshape(v_pool.shape)

    return jax.shard_map(per_device, mesh=mesh, in_specs=(seq_spec, full_spec, full_spec, full_spec, full_spec, full_spec, full_spec, pool_spec, pool_spec, table_spec, vec_spec, vec_spec, vec_spec), out_specs=(seq_spec, pool_spec, pool_spec), check_vma=False)
```

```python
import functools

import jax
import jax.numpy as jnp
from jax import lax
from jax.experimental import pallas as pl
from jax.experimental.pallas import tpu as pltpu
from jax.sharding import PartitionSpec as P

MESH = pl.DeviceIdType.MESH
ANY = pl.BlockSpec(memory_space=pl.ANY)
SMEM = pl.BlockSpec(memory_space=pltpu.SMEM)
VMEM = pl.BlockSpec(memory_space=pltpu.VMEM)
F32 = jnp.float32
BF16 = jnp.bfloat16
NEG = -1e30


def flat_id(n_cols):
    return lax.axis_index('kv2') * n_cols + lax.axis_index('kv')


def where_is(flat, n_cols):
    return {'kv2': flat // n_cols, 'kv': flat % n_cols}


def greet_all(n_dev, n_cols):
    me = flat_id(n_cols)
    barrier = pltpu.get_barrier_semaphore()

    @pl.loop(1, n_dev)
    def _(r):
        pl.semaphore_signal(barrier, inc=1, device_id=where_is((me + r) % n_dev, n_cols), device_id_type=MESH)

    pl.semaphore_wait(barrier, n_dev - 1)


def gather_all_kernel(n_dev, n_cols, x_ref, o_ref, local_sem, send_sem, recv_sem):
    me = flat_id(n_cols)
    greet_all(n_dev, n_cols)

    def copy(r, dst, slot):
        return pltpu.make_async_remote_copy(
            src_ref=x_ref, dst_ref=o_ref.at[slot], send_sem=send_sem.at[r], recv_sem=recv_sem.at[r],
            device_id=where_is(dst, n_cols), device_id_type=MESH)

    @pl.loop(1, n_dev)
    def _(r):
        copy(r, (me + r) % n_dev, me).start()

    own = pltpu.make_async_copy(x_ref, o_ref.at[me], local_sem)
    own.start()
    own.wait()

    @pl.loop(1, n_dev)
    def _(r):
        c = copy(r, (me + r) % n_dev, (me + n_dev - r) % n_dev)
        c.wait_send()
        c.wait_recv()


def row_gather_kernel(n_cols, x_ref, o_ref, local_sem, send_sem, recv_sem, fsend_sem, frecv_sem):
    n_chips = n_cols // 2
    kv = lax.axis_index('kv')
    chip, core = kv // 2, kv % 2
    mate = chip * 2 + 1 - core
    barrier = pltpu.get_barrier_semaphore()
    for r in range(1, n_chips):
        pl.semaphore_signal(barrier, inc=1, device_id={'kv': (chip + r) % n_chips * 2 + core}, device_id_type=MESH)
    pl.semaphore_signal(barrier, inc=1, device_id={'kv': mate}, device_id_type=MESH)
    pl.semaphore_wait(barrier, n_chips)

    def copy(r, dst, slot):
        return pltpu.make_async_remote_copy(
            src_ref=x_ref, dst_ref=o_ref.at[slot], send_sem=send_sem.at[r], recv_sem=recv_sem.at[r],
            device_id={'kv': dst}, device_id_type=MESH)

    def forward(r, slot):
        return pltpu.make_async_remote_copy(
            src_ref=o_ref.at[slot], dst_ref=o_ref.at[slot], send_sem=fsend_sem.at[r], recv_sem=frecv_sem.at[r],
            device_id={'kv': mate}, device_id_type=MESH)

    for r in range(1, n_chips):
        copy(r, (chip + r) % n_chips * 2 + core, kv).start()
    copy(0, mate, kv).start()
    own = pltpu.make_async_copy(x_ref, o_ref.at[kv], local_sem)
    own.start()
    own.wait()
    for r in range(1, n_chips):
        slot = (chip + n_chips - r) % n_chips * 2 + core
        copy(r, mate, slot).wait_recv()
        forward(r, slot).start()
    for r in range(1, n_chips):
        copy(r, mate, kv).wait_send()
        forward(r, (chip + n_chips - r) % n_chips * 2 + core).wait_send()
        forward(r, (chip + n_chips - r) % n_chips * 2 + 1 - core).wait_recv()
    c = copy(0, mate, mate)
    c.wait_send()
    c.wait_recv()


def return_kernel(n_cols, x_ref, ml_ref, out_ref, mate_o, mate_ml, sum_o, sum_ml, got_o, got_ml, dsend, drecv, send, recv):
    n_chips = n_cols // 2
    kv = lax.axis_index('kv')
    chip, core = kv // 2, kv % 2
    mate = chip * 2 + 1 - core
    seq_dev, rows, lanes = x_ref.shape[1:]
    heads = out_ref.shape[2]
    barrier = pltpu.get_barrier_semaphore()
    for r in range(1, n_chips):
        pl.semaphore_signal(barrier, inc=1, device_id={'kv': (chip + r) % n_chips * 2 + core}, device_id_type=MESH)
    pl.semaphore_signal(barrier, inc=1, device_id={'kv': mate}, device_id_type=MESH)
    pl.semaphore_wait(barrier, n_chips)

    def across(r, a):
        src, dst = ((x_ref, mate_o), (ml_ref, mate_ml))[a]
        return pltpu.make_async_remote_copy(
            src_ref=src.at[(chip + r) % n_chips * 2 + 1 - core], dst_ref=dst.at[r], send_sem=dsend.at[a, r], recv_sem=drecv.at[a, r],
            device_id={'kv': mate}, device_id_type=MESH)

    def home(r, a):
        src, dst = ((sum_o, got_o), (sum_ml, got_ml))[a]
        return pltpu.make_async_remote_copy(
            src_ref=src.at[r], dst_ref=dst.at[r], send_sem=send.at[a, r], recv_sem=recv.at[a, r],
            device_id={'kv': (chip + r) % n_chips * 2 + core}, device_id_type=MESH)

    order = sorted(range(1, n_chips), key=lambda r: -min(r, n_chips - r)) + [0]
    for r in order:
        for a in range(2):
            across(r, a).start()
    lane = lax.broadcasted_iota(jnp.int32, (8, lanes), 1)
    for r in order:
        slot = (chip + r) % n_chips * 2 + core
        to_o, to_ml = (sum_o, sum_ml) if r else (got_o, got_ml)
        for a in range(2):
            across(r, a).wait_recv()

        @pl.loop(0, seq_dev // 8)
        def _(g):
            some = pl.ds(pl.multiple_of(8 * g, 8), 8)
            ml1, ml2 = ml_ref[slot, some], mate_ml[r, some]
            top = jnp.maximum(ml1, ml2)
            w1, w2 = jnp.exp(ml1 - top), jnp.exp(ml2 - top)
            l = pltpu.roll(w1, rows, 1) * ml1 + pltpu.roll(w2, rows, 1) * ml2
            to_ml[r, some] = jnp.where(lane < rows, top, l)
            c1, c2 = w1.T, w2.T
            for t in range(8):
                b = 8 * g + t
                to_o[r, b] = c1[:rows, t:t + 1] * x_ref[slot, b] + c2[:rows, t:t + 1] * mate_o[r, b]

        if r:
            for a in range(2):
                home(r, a).start()
    for r in range(1, n_chips):
        for a in range(2):
            home(r, a).wait_recv()

    @pl.loop(0, seq_dev // 8)
    def _(g):
        some = pl.ds(pl.multiple_of(8 * g, 8), 8)
        mls = [got_ml[p, some] for p in range(n_chips)]
        top = functools.reduce(jnp.maximum, mls)
        ws = [jnp.exp(x - top) for x in mls]
        total = sum(w * pltpu.roll(x, lanes - rows, 1) for w, x in zip(ws, mls))
        cols = [(w / total).T for w in ws]
        for t in range(8):
            b = 8 * g + t
            acc = sum(c[:rows, t:t + 1] * got_o[p, b] for p, c in enumerate(cols)).astype(BF16)
            out_ref[0, b] = acc[:heads]
            out_ref[1, b] = acc[heads:]

    for r in range(n_chips):
        for a in range(2):
            across(r, a).wait_send()
            if r:
                home(r, a).wait_send()


def places_kernel(dims, who_ref, tab_ref, pages_ref, arrive_ref, most_ref, count):
    n_dev, n_cols, n_slots, seq_dev, n_moves, cap, page, magic, shift = dims
    n_chips = n_dev // 2
    o_dst = 3 * seq_dev + n_moves
    me = who_ref[0]
    base = me * n_slots

    @pl.loop(0, n_chips)
    def _(i):
        count[i] = 0

    @pl.loop(0, n_slots, unroll=8)
    def _(i):
        arrive_ref[n_slots + i] = -1

    @pl.loop(0, n_dev * cap, unroll=8)
    def _(i):
        pages_ref[i] = 0

    def device(d, landed):
        for j in range(n_moves):
            dst = tab_ref[d, o_dst + j]
            m = d * n_moves + j
            dd = (dst * magic) >> shift
            chip = dd >> 1
            n = count[chip]
            count[chip] = n + 1
            pages_ref[jnp.where(n < 2 * cap, chip * 2 * cap + n, n_dev * cap)] = m
            mine = dd == me
            s = dst - base
            arrive_ref[jnp.where(mine, landed, 3 * n_slots)] = s
            arrive_ref[jnp.where(mine, n_slots + s, 3 * n_slots)] = m
            arrive_ref[jnp.where(mine, 2 * n_slots + s, 3 * n_slots)] = n
            landed = landed + jnp.where(mine, 1, 0)
        return landed

    most_ref[1] = lax.fori_loop(0, n_dev, device, jnp.int32(0))
    most_ref[0] = lax.fori_loop(0, n_chips, lambda i, best: jnp.maximum(best, count[i]), jnp.int32(0))


def cells_kernel(dims, who_ref, tab_ref, none_ref, info_ref, used_ref, moved, seen, sem):
    n_dev, n_cols, n_slots, seq_dev, n_moves, cap, page, magic, shift = dims
    o_len, o_src, o_dst = 2 * seq_dev, 3 * seq_dev, 3 * seq_dev + n_moves
    row0 = who_ref[1]
    base = who_ref[0] * n_slots
    fill = pltpu.make_async_copy(none_ref, moved, sem)
    fill.start()

    seen[n_cols * seq_dev] = 0

    @pl.loop(0, n_cols * seq_dev, unroll=8)
    def _(i):
        seen[i] = 0

    @pl.loop(0, n_slots, unroll=8)
    def _(i):
        info_ref[i] = -1
        info_ref[n_slots + i] = -1

    fill.wait()

    @pl.loop(0, n_dev)
    def _(d):
        for j in range(n_moves):
            moved[tab_ref[d, o_src + j]] = tab_ref[d, o_dst + j]

    @pl.loop(0, n_cols)
    def _(h):
        @pl.loop(0, seq_dev, unroll=4)
        def _(i):
            b = h * seq_dev + i
            length = tab_ref[row0 + h, o_len + i]
            for j in range(2):
                e = tab_ref[row0 + h, 2 * i + j]
                e0 = jnp.maximum(e, 0)
                mv = moved[e0]
                s = jnp.where(mv >= 0, mv, e0) - base

                here = (e >= 0) & (s >= 0) & (s < n_slots)
                info_ref[jnp.where(here, n_slots + s, 4 * n_slots)] = b
                info_ref[jnp.where(here, 2 * n_slots + s, 4 * n_slots)] = length - page * j

    def visit(s, n):
        b = info_ref[n_slots + s]
        used = b >= 0
        b = jnp.where(used, b, n_cols * seq_dev)
        info_ref[jnp.where(used, n, 4 * n_slots)] = s
        info_ref[3 * n_slots + s] = seen[b]
        seen[b] = 1
        return n + jnp.where(used, 1, 0)

    used_ref[0] = lax.fori_loop(0, n_slots, visit, jnp.int32(0), unroll=4)


def pack_kernel(n_moves, src_ref, k_ref, v_ref, *rest):
    *outs, sem = rest

    def copies(m):
        s = src_ref[m]
        for layer, o_ref in enumerate(outs):
            half = o_ref.shape[0] // 2
            for a, pool in enumerate((k_ref, v_ref)):
                yield pltpu.make_async_copy(pool.at[s, layer], o_ref.at[pl.ds(a * half, half), m], sem.at[layer, a, m])

    for m in range(n_moves):
        for c in copies(m):
            c.start()
    for m in range(n_moves):
        for c in copies(m):
            c.wait()


def regroup_kernel(cap, pages_ref, x_ref, o_ref):
    @pl.loop(0, o_ref.shape[0])
    def _(d):
        for n in range(cap):
            o_ref[d, n] = x_ref[pages_ref[d * cap + n]]


def attend_kernel(dims, who_ref, arrive_ref, most_ref, info_ref, used_ref, q_ref, k_ref, v_ref, own_ref, mate_ref, slow_ref, *rest):
    layer, n_slots, cap, scale, quads, first = dims
    ko_ref, vo_ref, o_ref, ml_ref, kbuf, vbuf, in_sem, out_sem, arr_sem = rest if first else rest[2:]
    n_key, lanes = kbuf.shape[1] * kbuf.shape[2], kbuf.shape[3]
    n_ch = kbuf.shape[1]
    rows = o_ref.shape[1]
    over = most_ref[0] > 2 * cap
    core = who_ref[2]
    bufs = (kbuf, vbuf)
    part = pl.ds(layer * n_ch, n_ch)

    slabs = [pltpu.make_async_copy((k_ref, v_ref)[a].at[:, part], bufs[a], in_sem.at[a]) for a in range(2)]
    for c in slabs:
        c.start()
    o_ref[...] = jnp.zeros_like(o_ref)
    ml_lane = lax.broadcasted_iota(jnp.int32, ml_ref.shape, 1)
    ml_ref[...] = jnp.where(ml_lane < rows, NEG, 0.0)
    for c in slabs:
        c.wait()

    def arrival(i, a, src):
        return pltpu.make_async_copy(src, bufs[a].at[arrive_ref[i]], arr_sem.at[a, i])

    @pl.loop(0, most_ref[1])
    def _(i):
        s = arrive_ref[i]
        n = arrive_ref[2 * n_slots + s]
        half = jnp.where(n >= cap, 1, 0)
        pos = n - half * cap

        def go(cond, src_of):
            @pl.when(cond)
            def _():
                for a in range(2):
                    arrival(i, a, src_of(pl.ds(a * n_ch, n_ch))).start()

        go(over, lambda some: slow_ref.at[layer, s, some])
        go(jnp.logical_not(over) & (half == core), lambda some: own_ref.at[some, pos])
        go(jnp.logical_not(over) & (half != core), lambda some: mate_ref.at[some, pos])

    @pl.loop(0, most_ref[1])
    def _(i):
        for a in range(2):
            arrival(i, a, own_ref.at[pl.ds(a * n_ch, n_ch), 0]).wait()

    n_used = used_ref[0]
    tile = kbuf.shape[2]
    tile_row = lax.broadcasted_iota(jnp.int32, (tile, lanes), 0)

    @pl.loop(0, n_used)
    def _(i):
        s = info_ref[i]
        lim = info_ref[2 * n_slots + s]

        @pl.when(lim < n_key // 2)
        def _():
            fresh = q_ref[info_ref[n_slots + s], rows:].astype(F32)
            row0 = 2 * lim
            for c in (row0 // tile, jnp.minimum((row0 + 3) // tile, n_ch - 1)):
                at = tile_row + c * tile - row0
                for a, buf in enumerate(bufs):
                    x = buf[s, c].astype(F32)
                    for r in range(4):
                        x = jnp.where(at == r, fresh[4 * a + r:4 * a + r + 1], x)
                    buf[s, c] = x.astype(BF16)

    outs = [pltpu.make_async_copy(bufs[a], (ko_ref, vo_ref)[a].at[:, part], out_sem.at[a]) for a in range(2)]
    for c in outs:
        c.start()

    lane = lax.broadcasted_iota(jnp.int32, (rows, n_key), 1)
    row = lax.broadcasted_iota(jnp.int32, (rows, n_key), 0)
    own_head = (lane & 1) == ((row >> 3) & 1)
    late = (lane >> 1) - (row >> 4)
    out_lane = lax.broadcasted_iota(jnp.int32, (rows, lanes), 1)
    out_row = lax.broadcasted_iota(jnp.int32, (rows, lanes), 0)
    nothing = jnp.zeros((rows, n_key), BF16)

    @pl.loop(0, (n_used + 4 * quads - 1) // (4 * quads))
    def _(u):
        done = []
        for quad in range(quads):
            facts = []
            for t in range(4):
                i = (u * quads + quad) * 4 + t
                listed = info_ref[jnp.minimum(i, n_slots - 1)]
                used = (i < n_slots) & (listed >= 0)
                s = jnp.where(used, listed, 0)
                facts.append((s, used, jnp.maximum(info_ref[n_slots + s], 0), info_ref[2 * n_slots + s], info_ref[3 * n_slots + s]))
            q = jnp.concatenate([q_ref[f[2], :rows] for f in facts], axis=0)
            k = jnp.concatenate([kbuf[f[0]].reshape(n_key, lanes) for f in facts], axis=0)
            v = jnp.concatenate([vbuf[f[0]].reshape(n_key, lanes) for f in facts], axis=0)
            scores = lax.dot_general(q, k, (((1,), (1,)), ((), ())), preferred_element_type=F32)
            ps, stats = [], []
            for t, (s, used, b, lim, again) in enumerate(facts):
                sc = scores[t * rows:(t + 1) * rows, t * n_key:(t + 1) * n_key] * scale
                sc = jnp.where(own_head & (late <= lim), sc, NEG)
                m = jnp.max(sc, axis=1, keepdims=True)
                p = jnp.exp(sc - m)
                stats.append((m, jnp.sum(p, axis=1, keepdims=True)))
                ps.append(jnp.concatenate([p.astype(BF16) if x == t else nothing for x in range(4)], axis=1))
            o = jnp.dot(jnp.concatenate(ps, axis=0), v, preferred_element_type=F32)
            for t, (s, used, b, lim, again) in enumerate(facts):
                done.append((used, b, *stats[t], o[t * rows:(t + 1) * rows], again))
        for used, b0, m, l, o, again in done:
            def put(m, l, o):
                o_ref[b0] = o
                ml = jnp.where(out_lane == out_row, m, 0.0) + jnp.where(out_lane == out_row + rows, l, 0.0)
                ml_ref[pl.ds(b0, 1)] = jnp.sum(ml, axis=0, keepdims=True)

            @pl.when(used & (again == 0))
            def _():
                put(m, l, o)

            @pl.when(used & (again > 0))
            def _():
                old = jnp.broadcast_to(ml_ref[pl.ds(b0, 1)], (rows, lanes))
                m1 = jnp.sum(jnp.where(out_lane == out_row, old, 0.0), axis=1, keepdims=True)
                l1 = jnp.sum(jnp.where(out_lane == out_row + rows, old, 0.0), axis=1, keepdims=True)
                mm = jnp.maximum(m, m1)
                w, w1 = jnp.exp(m - mm), jnp.exp(m1 - mm)
                put(mm, l * w + l1 * w1, o * w + o_ref[b0] * w1)

    for c in outs:
        c.wait()


def mlp_kernel(layer, depth, attn_ref, hid_ref, wo_ref, up_ref, dn_ref, out_ref, abuf, bbuf, x_all, u, acc, got, a_sem, b_sem, send, recv):
    kv = lax.axis_index('kv')
    core = kv % 2
    mate = kv + 1 - 2 * core
    width, tile = abuf.shape[1:]
    n_out = width // tile
    n_up = -(-up_ref.shape[2] // (2 * tile))
    base = core * (up_ref.shape[2] - n_up * tile)
    both = 2 * n_up * tile - up_ref.shape[2]
    chunk = 256

    def cols(t):
        return pl.ds(pl.multiple_of(base + t * tile, chunk), tile)

    def load_out(n):
        return pltpu.make_async_copy(wo_ref.at[layer, :, pl.ds(n * tile, tile)], abuf.at[n % depth], a_sem.at[n % depth])

    def load_up(t):
        slot = (t + n_out) % depth
        return pltpu.make_async_copy(up_ref.at[layer, :, cols(t)], abuf.at[slot], a_sem.at[slot])

    def load_down(t):
        slot = t % depth
        return pltpu.make_async_copy(dn_ref.at[layer, cols(t), :], bbuf.at[slot], b_sem.at[slot])

    for n in range(min(depth, n_out)):
        load_out(n).start()
    for t in range(depth):
        load_down(t).start()
    barrier = pltpu.get_barrier_semaphore()
    pl.semaphore_signal(barrier, inc=1, device_id={'kv': mate}, device_id_type=MESH)
    pl.semaphore_wait(barrier, 1)

    def across(src, dst, i):
        return pltpu.make_async_remote_copy(
            src_ref=src, dst_ref=dst, send_sem=send.at[i], recv_sem=recv.at[i], device_id={'kv': mate}, device_id_type=MESH)

    for n in range(n_out):
        load_out(n).wait()
        part = slice(n * tile, (n + 1) * tile)
        y = jnp.dot(attn_ref[...], abuf[n % depth], preferred_element_type=F32)
        x_all[core, :, part] = (hid_ref[:, part].astype(F32) + y).astype(BF16)
        later = n + depth
        if later < n_out:
            load_out(later).start()
        else:
            load_up(later - n_out).start()
    share = across(x_all.at[core], x_all.at[core], 0)
    share.start()
    acc[...] = jnp.zeros_like(acc)
    share.wait_send()
    across(x_all.at[core], x_all.at[1 - core], 0).wait_recv()

    @pl.loop(0, n_up)
    def _(t):
        slot = (t + n_out) % depth
        load_up(t).wait()
        x = x_all[...].reshape(-1, width)
        for c in range(tile // chunk):
            part = slice(c * chunk, (c + 1) * chunk)
            y = jax.nn.gelu(jnp.dot(x, abuf[slot, :, part], preferred_element_type=F32)).astype(BF16)
            if c * chunk < both:
                y = jnp.where((core == 1) & (t == 0), jnp.zeros_like(y), y)
            u[:, part] = y

        @pl.when(t + depth < n_up)
        def _():
            load_up(t + depth).start()

        load_down(t).wait()
        for c in range(width // tile):
            part = slice(c * tile, (c + 1) * tile)
            y = jnp.dot(u[...], bbuf[t % depth, :, part], preferred_element_type=F32)
            acc[:, :, part] += y.reshape(acc.shape[0], acc.shape[1], tile)

        @pl.when(t + depth < n_up)
        def _():
            load_down(t + depth).start()

    give = across(acc.at[1 - core], got, 1)
    give.start()
    give.wait()
    out_ref[...] = (x_all[core].astype(F32) + (acc[core] + got[...])).astype(BF16)


def blank_kernel(o_ref):
    pass


def sems(*shape):
    return pltpu.SemaphoreType.DMA(shape)


def comm(cid, mib=None):
    return pltpu.CompilerParams(collective_id=cid, has_side_effects=True, **({'vmem_limit_bytes': mib << 20} if mib else {}))


def solution(mesh):
    n_rows = mesh.shape['kv2']
    n_cols = mesh.shape['kv']
    n_dev = n_rows * n_cols
    dev_axes = ('rep', 'kv2', 'kv')
    seq_spec = P(None, dev_axes, None)
    pool_spec = P(dev_axes, None, None, None, None)
    table_spec = P(dev_axes, None)
    vec_spec = P(dev_axes)
    full_spec = P()

    def per_device(x_embed, w_query, w_key, w_value, w_out, w_up, w_down, k_pool, v_pool, old_table, seq_len, src_slot, dst_slot):
        n_slots, layers, page, kv_heads, head_dim = k_pool.shape
        heads = w_query.shape[2] // head_dim
        n_steps, seq_dev, width = x_embed.shape
        n_moves = src_slot.shape[0]
        row_seqs = seq_dev * n_cols
        rows = n_steps * heads
        key_rows = page * kv_heads
        tile = 8
        n_ch = key_rows // tile
        chunks = 2 * n_ch
        cap = 20
        assert chunks == n_dev and rows == 32 and old_table.shape[1] == 2
        shift = 18
        magic = -(-(1 << shift) // n_slots)
        assert all((s * magic) >> shift == s // n_slots for s in range(n_dev * n_slots))
        me = flat_id(n_cols)
        who = jnp.stack([me, lax.axis_index('kv2') * n_cols, lax.axis_index('kv') % 2]).astype(jnp.int32)

        kp = k_pool.reshape(n_slots, layers, n_ch, tile, head_dim)
        vp = v_pool.reshape(n_slots, layers, n_ch, tile, head_dim)
        kp4 = k_pool.reshape(n_slots, layers * n_ch, tile, head_dim)
        vp4 = v_pool.reshape(n_slots, layers * n_ch, tile, head_dim)
        packed = pl.pallas_call(
            functools.partial(pack_kernel, n_moves),
            out_shape=[jax.ShapeDtypeStruct((chunks, n_moves, tile, head_dim), BF16)] * layers,
            in_specs=[SMEM, ANY, ANY], out_specs=[VMEM] * layers,
            scratch_shapes=[sems(layers, 2, n_moves)], name='pack_pages')(src_slot - me * n_slots, kp, vp)
        after = lax.optimization_barrier

        mine = jnp.concatenate([old_table.reshape(-1), seq_len, src_slot, dst_slot])
        mine = jnp.pad(mine, (0, 128 - mine.shape[0])).reshape(1, 128)
        tab = pl.pallas_call(
            functools.partial(gather_all_kernel, n_dev, n_cols),
            out_shape=jax.ShapeDtypeStruct((n_dev, 1, 128), jnp.int32),
            in_specs=[VMEM], out_specs=VMEM,
            scratch_shapes=[pltpu.SemaphoreType.DMA, sems(n_dev), sems(n_dev)],
            compiler_params=comm(0), name='gather_tables')(mine)

        tab = tab.reshape(n_dev, 128)
        moving, tab = after((packed[0], tab))
        spread = lax.all_to_all(moving, ('kv2', 'kv'), 0, 0, tiled=True)
        dims = (n_dev, n_cols, n_slots, seq_dev, n_moves, cap, page, magic, shift)
        pages, arrive, most = pl.pallas_call(
            functools.partial(places_kernel, dims),
            out_shape=(jax.ShapeDtypeStruct((n_dev * cap + 1,), jnp.int32), jax.ShapeDtypeStruct((3 * n_slots + 1,), jnp.int32),
                       jax.ShapeDtypeStruct((2,), jnp.int32)),
            in_specs=[SMEM, SMEM], out_specs=(SMEM, SMEM, SMEM),
            scratch_shapes=[pltpu.SMEM((n_dev // 2,), jnp.int32)], name='places')(who, tab)

        def regroup(spread, name):
            return pl.pallas_call(
                functools.partial(regroup_kernel, cap),
                out_shape=jax.ShapeDtypeStruct((n_dev, cap, tile, head_dim), BF16),
                in_specs=[SMEM, VMEM], out_specs=VMEM, name=name)(pages, spread.reshape(n_dev * n_moves, tile, head_dim))

        def deliver(grouped):
            return lax.all_to_all(grouped, ('kv2', 'kv'), 0, 0, tiled=True)

        def to_mate(own):
            return lax.ppermute(own, 'kv', [(i, i ^ 1) for i in range(n_cols)])

        def all_pages():
            found = []
            for p in packed:
                everything = lax.all_gather(p.swapaxes(0, 1), ('kv2', 'kv'), tiled=True)
                found.append(everything[jnp.maximum(arrive[n_slots:2 * n_slots], 0)])
            return jnp.stack(found)

        def no_pages():
            return pl.pallas_call(
                blank_kernel, out_shape=jax.ShapeDtypeStruct((layers, n_slots, chunks, tile, head_dim), BF16), out_specs=ANY,
                name='blank')()

        slow = lax.cond(most[0] > 2 * cap, all_pages, no_pages)

        hidden = x_embed.reshape(n_steps * seq_dev, width)
        k_out = v_out = None
        for layer in range(layers):
            query = jnp.dot(hidden, w_query[layer], preferred_element_type=F32).astype(BF16)
            k_new = jnp.dot(hidden, w_key[layer], preferred_element_type=F32).astype(BF16)
            v_new = jnp.dot(hidden, w_value[layer], preferred_element_type=F32).astype(BF16)

            def by_seq(x):
                return x.reshape(n_steps, seq_dev, -1, head_dim).swapaxes(0, 1).reshape(seq_dev, -1, head_dim)

            load = jnp.concatenate([by_seq(query), by_seq(k_new), by_seq(v_new)], axis=1)
            q_rows = load.shape[1]
            if layer == 0:
                spread, load, pages = after((spread, load, pages))
                grouped, load, tab = after((regroup(spread, 'regroup_pages_0'), load, tab))
                own = deliver(grouped)
                info, n_used = pl.pallas_call(
                    functools.partial(cells_kernel, dims),
                    out_shape=(jax.ShapeDtypeStruct((4 * n_slots + 1,), jnp.int32), jax.ShapeDtypeStruct((1,), jnp.int32)),
                    in_specs=[SMEM, SMEM, ANY], out_specs=(SMEM, SMEM),
                    scratch_shapes=[pltpu.SMEM((n_dev * n_slots,), jnp.int32), pltpu.SMEM((row_seqs + 1,), jnp.int32), pltpu.SemaphoreType.DMA],
                    name='cells')(who, tab, jnp.full((n_dev * n_slots,), -1, jnp.int32))
                pool_shape = jax.ShapeDtypeStruct(kp4.shape, BF16)
                load, info = after((load, info))
            else:
                own, load = after((own, load))
                mate = to_mate(own)
            n_chips = n_cols // 2
            q_row = pl.pallas_call(
                functools.partial(row_gather_kernel, n_cols),
                out_shape=jax.ShapeDtypeStruct((n_cols, seq_dev, q_rows, head_dim), BF16),
                in_specs=[VMEM], out_specs=VMEM,
                scratch_shapes=[pltpu.SemaphoreType.DMA, sems(n_chips), sems(n_chips), sems(n_chips), sems(n_chips)],
                compiler_params=comm(3 + layer, 40), name=f'gather_queries_{layer}')(load)

            first = layer == 0
            if first:
                own, q_row = after((own, q_row))
                mate = to_mate(own)
            last = layer == layers - 1
            if not last:
                moving, q_row = after((packed[layer + 1], q_row))
                spread = lax.all_to_all(moving, ('kv2', 'kv'), 0, 0, tiled=True)
            carried = () if first else (k_out, v_out)
            k_out, v_out, part, ml = pl.pallas_call(
                functools.partial(attend_kernel, (layer, n_slots, cap, head_dim ** -0.5, 2, first)),
                in_specs=[SMEM] * 5 + [VMEM] + [ANY] * (5 + len(carried)),
                out_specs=[ANY, ANY, VMEM, VMEM],
                out_shape=[pool_shape, pool_shape, jax.ShapeDtypeStruct((row_seqs, rows, head_dim), F32),
                           jax.ShapeDtypeStruct((row_seqs, head_dim), F32)],
                scratch_shapes=[pltpu.VMEM((n_slots, n_ch, tile, head_dim), BF16), pltpu.VMEM((n_slots, n_ch, tile, head_dim), BF16),
                                sems(2), sems(2), sems(2, n_slots)],
                input_output_aliases={} if first else {11: 0, 12: 1},
                compiler_params=pltpu.CompilerParams(vmem_limit_bytes=46 << 20), name=f'attend_{layer}')(who, arrive, most, info, n_used, q_row.reshape(row_seqs, q_rows, head_dim), kp4, vp4,
                                        own, mate, slow, *carried)

            parts, parts_ml = (n_chips, seq_dev, rows, head_dim), (n_chips, seq_dev, head_dim)
            attn = pl.pallas_call(
                functools.partial(return_kernel, n_cols),
                out_shape=jax.ShapeDtypeStruct((n_steps, seq_dev, heads, head_dim), BF16),
                in_specs=[VMEM, VMEM], out_specs=VMEM,
                scratch_shapes=[pltpu.VMEM(shape, F32) for _ in range(3) for shape in (parts, parts_ml)] + [sems(2, n_chips)] * 4,
                compiler_params=comm(5 + layer, 40), name=f'return_{layer}')(
                    part.reshape(n_cols, seq_dev, rows, head_dim), ml.reshape(n_cols, seq_dev, head_dim))
            attn_out = attn.reshape(n_steps * seq_dev, heads * head_dim)
            n_tok = n_steps * seq_dev
            if not last:
                spread, attn_out = after((spread, attn_out))
                grouped, attn_out = after((regroup(spread, f'regroup_pages_{layer + 1}'), attn_out))
                own = deliver(grouped)
            depth, wide = 4, 512
            assert w_up.shape[2] % 256 == 0 and width % wide == 0
            hidden = pl.pallas_call(
                functools.partial(mlp_kernel, layer, depth),
                out_shape=jax.ShapeDtypeStruct((n_tok, width), BF16),
                in_specs=[VMEM, VMEM, ANY, ANY, ANY], out_specs=VMEM,
                scratch_shapes=[pltpu.VMEM((depth, width, wide), BF16), pltpu.VMEM((depth, wide, width), BF16),
                                pltpu.VMEM((2, n_tok, width), BF16), pltpu.VMEM((2 * n_tok, wide), BF16),
                                pltpu.VMEM((2, n_tok, width), F32), pltpu.VMEM((n_tok, width), F32),
                                sems(depth), sems(depth), sems(2), sems(2)],
                compiler_params=comm(7 + layer, 57), name=f'mlp_{layer}')(attn_out, hidden, w_out, w_up, w_down)
        return hidden.reshape(x_embed.shape), k_out.reshape(k_pool.shape), v_out.reshape(v_pool.shape)

    return jax.shard_map(per_device, mesh=mesh, in_specs=(seq_spec, full_spec, full_spec, full_spec, full_spec, full_spec, full_spec, pool_spec, pool_spec, table_spec, vec_spec, vec_spec, vec_spec), out_specs=(seq_spec, pool_spec, pool_spec), check_vma=False)
```

```python
import functools

import jax
import jax.numpy as jnp
from jax import lax
from jax.experimental import pallas as pl
from jax.experimental.pallas import tpu as pltpu
from jax.sharding import PartitionSpec as P

MESH = pl.DeviceIdType.MESH
ANY = pl.BlockSpec(memory_space=pl.ANY)
SMEM = pl.BlockSpec(memory_space=pltpu.SMEM)
VMEM = pl.BlockSpec(memory_space=pltpu.VMEM)
F32 = jnp.float32
BF16 = jnp.bfloat16
NEG = -1e30


def flat_id(n_cols):
    return lax.axis_index('kv2') * n_cols + lax.axis_index('kv')


def where_is(flat, n_cols):
    return {'kv2': flat // n_cols, 'kv': flat % n_cols}


def greet_all(n_dev, n_cols):
    me = flat_id(n_cols)
    barrier = pltpu.get_barrier_semaphore()

    @pl.loop(1, n_dev)
    def _(r):
        pl.semaphore_signal(barrier, inc=1, device_id=where_is((me + r) % n_dev, n_cols), device_id_type=MESH)

    pl.semaphore_wait(barrier, n_dev - 1)


def gather_all_kernel(n_dev, n_cols, x_ref, o_ref, local_sem, send_sem, recv_sem):
    me = flat_id(n_cols)
    greet_all(n_dev, n_cols)

    def copy(r, dst, slot):
        return pltpu.make_async_remote_copy(
            src_ref=x_ref, dst_ref=o_ref.at[slot], send_sem=send_sem.at[r], recv_sem=recv_sem.at[r],
            device_id=where_is(dst, n_cols), device_id_type=MESH)

    @pl.loop(1, n_dev)
    def _(r):
        copy(r, (me + r) % n_dev, me).start()

    own = pltpu.make_async_copy(x_ref, o_ref.at[me], local_sem)
    own.start()
    own.wait()

    @pl.loop(1, n_dev)
    def _(r):
        c = copy(r, (me + r) % n_dev, (me + n_dev - r) % n_dev)
        c.wait_send()
        c.wait_recv()


def row_gather_kernel(n_cols, x_ref, o_ref, local_sem, send_sem, recv_sem, fsend_sem, frecv_sem):
    n_chips = n_cols // 2
    kv = lax.axis_index('kv')
    chip, core = kv // 2, kv % 2
    mate = chip * 2 + 1 - core
    barrier = pltpu.get_barrier_semaphore()
    for r in range(1, n_chips):
        pl.semaphore_signal(barrier, inc=1, device_id={'kv': (chip + r) % n_chips * 2 + core}, device_id_type=MESH)
    pl.semaphore_signal(barrier, inc=1, device_id={'kv': mate}, device_id_type=MESH)
    pl.semaphore_wait(barrier, n_chips)

    def copy(r, dst, slot):
        return pltpu.make_async_remote_copy(
            src_ref=x_ref, dst_ref=o_ref.at[slot], send_sem=send_sem.at[r], recv_sem=recv_sem.at[r],
            device_id={'kv': dst}, device_id_type=MESH)

    def forward(r, slot):
        return pltpu.make_async_remote_copy(
            src_ref=o_ref.at[slot], dst_ref=o_ref.at[slot], send_sem=fsend_sem.at[r], recv_sem=frecv_sem.at[r],
            device_id={'kv': mate}, device_id_type=MESH)

    for r in range(1, n_chips):
        copy(r, (chip + r) % n_chips * 2 + core, kv).start()
    copy(0, mate, kv).start()
    own = pltpu.make_async_copy(x_ref, o_ref.at[kv], local_sem)
    own.start()
    own.wait()
    for r in range(1, n_chips):
        slot = (chip + n_chips - r) % n_chips * 2 + core
        copy(r, mate, slot).wait_recv()
        forward(r, slot).start()
    for r in range(1, n_chips):
        copy(r, mate, kv).wait_send()
        forward(r, (chip + n_chips - r) % n_chips * 2 + core).wait_send()
        forward(r, (chip + n_chips - r) % n_chips * 2 + 1 - core).wait_recv()
    c = copy(0, mate, mate)
    c.wait_send()
    c.wait_recv()


def return_kernel(n_cols, x_ref, ml_ref, out_ref, mate_o, mate_ml, sum_o, sum_ml, got_o, got_ml, dsend, drecv, send, recv):
    n_chips = n_cols // 2
    kv = lax.axis_index('kv')
    chip, core = kv // 2, kv % 2
    mate = chip * 2 + 1 - core
    seq_dev, rows, lanes = x_ref.shape[1:]
    heads = out_ref.shape[2]
    barrier = pltpu.get_barrier_semaphore()
    for r in range(1, n_chips):
        pl.semaphore_signal(barrier, inc=1, device_id={'kv': (chip + r) % n_chips * 2 + core}, device_id_type=MESH)
    pl.semaphore_signal(barrier, inc=1, device_id={'kv': mate}, device_id_type=MESH)
    pl.semaphore_wait(barrier, n_chips)

    def across(r, a):
        src, dst = ((x_ref, mate_o), (ml_ref, mate_ml))[a]
        return pltpu.make_async_remote_copy(
            src_ref=src.at[(chip + r) % n_chips * 2 + 1 - core], dst_ref=dst.at[r], send_sem=dsend.at[a, r], recv_sem=drecv.at[a, r],
            device_id={'kv': mate}, device_id_type=MESH)

    def home(r, a):
        src, dst = ((sum_o, got_o), (sum_ml, got_ml))[a]
        return pltpu.make_async_remote_copy(
            src_ref=src.at[r], dst_ref=dst.at[r], send_sem=send.at[a, r], recv_sem=recv.at[a, r],
            device_id={'kv': (chip + r) % n_chips * 2 + core}, device_id_type=MESH)

    order = sorted(range(1, n_chips), key=lambda r: -min(r, n_chips - r)) + [0]
    for r in order:
        for a in range(2):
            across(r, a).start()
    lane = lax.broadcasted_iota(jnp.int32, (8, lanes), 1)
    for r in order:
        slot = (chip + r) % n_chips * 2 + core
        to_o, to_ml = (sum_o, sum_ml) if r else (got_o, got_ml)
        for a in range(2):
            across(r, a).wait_recv()

        @pl.loop(0, seq_dev // 8)
        def _(g):
            some = pl.ds(pl.multiple_of(8 * g, 8), 8)
            ml1, ml2 = ml_ref[slot, some], mate_ml[r, some]
            top = jnp.maximum(ml1, ml2)
            w1, w2 = jnp.exp(ml1 - top), jnp.exp(ml2 - top)
            l = pltpu.roll(w1, rows, 1) * ml1 + pltpu.roll(w2, rows, 1) * ml2
            to_ml[r, some] = jnp.where(lane < rows, top, l)
            c1, c2 = w1.T, w2.T
            for t in range(8):
                b = 8 * g + t
                to_o[r, b] = c1[:rows, t:t + 1] * x_ref[slot, b] + c2[:rows, t:t + 1] * mate_o[r, b]

        if r:
            for a in range(2):
                home(r, a).start()
    for r in range(1, n_chips):
        for a in range(2):
            home(r, a).wait_recv()

    @pl.loop(0, seq_dev // 8)
    def _(g):
        some = pl.ds(pl.multiple_of(8 * g, 8), 8)
        mls = [got_ml[p, some] for p in range(n_chips)]
        top = functools.reduce(jnp.maximum, mls)
        ws = [jnp.exp(x - top) for x in mls]
        total = sum(w * pltpu.roll(x, lanes - rows, 1) for w, x in zip(ws, mls))
        cols = [(w / total).T for w in ws]
        for t in range(8):
            b = 8 * g + t
            acc = sum(c[:rows, t:t + 1] * got_o[p, b] for p, c in enumerate(cols)).astype(BF16)
            out_ref[0, b] = acc[:heads]
            out_ref[1, b] = acc[heads:]

    for r in range(n_chips):
        for a in range(2):
            across(r, a).wait_send()
            if r:
                home(r, a).wait_send()


def places_kernel(dims, who_ref, tab_ref, pages_ref, arrive_ref, most_ref, count):
    n_dev, n_cols, n_slots, seq_dev, n_moves, cap, page, magic, shift = dims
    n_chips = n_dev // 2
    o_dst = 3 * seq_dev + n_moves
    me = who_ref[0]
    base = me * n_slots

    @pl.loop(0, n_chips)
    def _(i):
        count[i] = 0

    @pl.loop(0, n_slots, unroll=8)
    def _(i):
        arrive_ref[n_slots + i] = -1

    @pl.loop(0, n_dev * cap, unroll=8)
    def _(i):
        pages_ref[i] = 0

    def device(d, landed):
        for j in range(n_moves):
            dst = tab_ref[d, o_dst + j]
            m = d * n_moves + j
            dd = (dst * magic) >> shift
            chip = dd >> 1
            n = count[chip]
            count[chip] = n + 1
            pages_ref[jnp.where(n < 2 * cap, chip * 2 * cap + n, n_dev * cap)] = m
            mine = dd == me
            s = dst - base
            arrive_ref[jnp.where(mine, landed, 3 * n_slots)] = s
            arrive_ref[jnp.where(mine, n_slots + s, 3 * n_slots)] = m
            arrive_ref[jnp.where(mine, 2 * n_slots + s, 3 * n_slots)] = n
            landed = landed + jnp.where(mine, 1, 0)
        return landed

    most_ref[1] = lax.fori_loop(0, n_dev, device, jnp.int32(0))
    most_ref[0] = lax.fori_loop(0, n_chips, lambda i, best: jnp.maximum(best, count[i]), jnp.int32(0))


def cells_kernel(dims, who_ref, tab_ref, none_ref, info_ref, used_ref, moved, seen, sem):
    n_dev, n_cols, n_slots, seq_dev, n_moves, cap, page, magic, shift = dims
    o_len, o_src, o_dst = 2 * seq_dev, 3 * seq_dev, 3 * seq_dev + n_moves
    row0 = who_ref[1]
    base = who_ref[0] * n_slots
    fill = pltpu.make_async_copy(none_ref, moved, sem)
    fill.start()

    seen[n_cols * seq_dev] = 0

    @pl.loop(0, n_cols * seq_dev, unroll=8)
    def _(i):
        seen[i] = 0

    @pl.loop(0, n_slots, unroll=8)
    def _(i):
        info_ref[i] = -1
        info_ref[n_slots + i] = -1

    fill.wait()

    @pl.loop(0, n_dev)
    def _(d):
        for j in range(n_moves):
            moved[tab_ref[d, o_src + j]] = tab_ref[d, o_dst + j]

    @pl.loop(0, n_cols)
    def _(h):
        @pl.loop(0, seq_dev, unroll=4)
        def _(i):
            b = h * seq_dev + i
            length = tab_ref[row0 + h, o_len + i]
            for j in range(2):
                e = tab_ref[row0 + h, 2 * i + j]
                e0 = jnp.maximum(e, 0)
                mv = moved[e0]
                s = jnp.where(mv >= 0, mv, e0) - base

                here = (e >= 0) & (s >= 0) & (s < n_slots)
                info_ref[jnp.where(here, n_slots + s, 4 * n_slots)] = b
                info_ref[jnp.where(here, 2 * n_slots + s, 4 * n_slots)] = length - page * j

    def visit(s, n):
        b = info_ref[n_slots + s]
        used = b >= 0
        b = jnp.where(used, b, n_cols * seq_dev)
        info_ref[jnp.where(used, n, 4 * n_slots)] = s
        info_ref[3 * n_slots + s] = seen[b]
        seen[b] = 1
        return n + jnp.where(used, 1, 0)

    used_ref[0] = lax.fori_loop(0, n_slots, visit, jnp.int32(0), unroll=4)


def pack_kernel(n_moves, src_ref, k_ref, v_ref, *rest):
    *outs, sem = rest

    def copies(m):
        s = src_ref[m]
        for layer, o_ref in enumerate(outs):
            half = o_ref.shape[0] // 2
            for a, pool in enumerate((k_ref, v_ref)):
                yield pltpu.make_async_copy(pool.at[s, layer], o_ref.at[pl.ds(a * half, half), m], sem.at[layer, a, m])

    for m in range(n_moves):
        for c in copies(m):
            c.start()
    for m in range(n_moves):
        for c in copies(m):
            c.wait()


def regroup_kernel(cap, pages_ref, x_ref, o_ref):
    @pl.loop(0, o_ref.shape[0])
    def _(d):
        for n in range(cap):
            o_ref[d, n] = x_ref[pages_ref[d * cap + n]]


def attend_kernel(dims, who_ref, arrive_ref, most_ref, info_ref, used_ref, q_ref, k_ref, v_ref, own_ref, mate_ref, slow_ref, *rest):
    layer, n_slots, cap, scale, quads, first = dims
    ko_ref, vo_ref, o_ref, ml_ref, kbuf, vbuf, in_sem, out_sem, arr_sem = rest if first else rest[2:]
    n_key, lanes = kbuf.shape[1] * kbuf.shape[2], kbuf.shape[3]
    n_ch = kbuf.shape[1]
    rows = o_ref.shape[1]
    over = most_ref[0] > 2 * cap
    core = who_ref[2]
    bufs = (kbuf, vbuf)
    part = pl.ds(layer * n_ch, n_ch)

    slabs = [pltpu.make_async_copy((k_ref, v_ref)[a].at[:, part], bufs[a], in_sem.at[a]) for a in range(2)]
    for c in slabs:
        c.start()
    o_ref[...] = jnp.zeros_like(o_ref)
    ml_lane = lax.broadcasted_iota(jnp.int32, ml_ref.shape, 1)
    ml_ref[...] = jnp.where(ml_lane < rows, NEG, 0.0)
    for c in slabs:
        c.wait()

    def arrival(i, a, src):
        return pltpu.make_async_copy(src, bufs[a].at[arrive_ref[i]], arr_sem.at[a, i])

    @pl.loop(0, most_ref[1])
    def _(i):
        s = arrive_ref[i]
        n = arrive_ref[2 * n_slots + s]
        half = jnp.where(n >= cap, 1, 0)
        pos = n - half * cap

        def go(cond, src_of):
            @pl.when(cond)
            def _():
                for a in range(2):
                    arrival(i, a, src_of(pl.ds(a * n_ch, n_ch))).start()

        go(over, lambda some: slow_ref.at[layer, s, some])
        go(jnp.logical_not(over) & (half == core), lambda some: own_ref.at[some, pos])
        go(jnp.logical_not(over) & (half != core), lambda some: mate_ref.at[some, pos])

    @pl.loop(0, most_ref[1])
    def _(i):
        for a in range(2):
            arrival(i, a, own_ref.at[pl.ds(a * n_ch, n_ch), 0]).wait()

    n_used = used_ref[0]
    tile = kbuf.shape[2]
    tile_row = lax.broadcasted_iota(jnp.int32, (tile, lanes), 0)

    @pl.loop(0, n_used)
    def _(i):
        s = info_ref[i]
        lim = info_ref[2 * n_slots + s]

        @pl.when(lim < n_key // 2)
        def _():
            fresh = q_ref[info_ref[n_slots + s], rows:].astype(F32)
            row0 = 2 * lim
            for c in (row0 // tile, jnp.minimum((row0 + 3) // tile, n_ch - 1)):
                at = tile_row + c * tile - row0
                for a, buf in enumerate(bufs):
                    x = buf[s, c].astype(F32)
                    for r in range(4):
                        x = jnp.where(at == r, fresh[4 * a + r:4 * a + r + 1], x)
                    buf[s, c] = x.astype(BF16)

    outs = [pltpu.make_async_copy(bufs[a], (ko_ref, vo_ref)[a].at[:, part], out_sem.at[a]) for a in range(2)]
    for c in outs:
        c.start()

    lane = lax.broadcasted_iota(jnp.int32, (rows, n_key), 1)
    row = lax.broadcasted_iota(jnp.int32, (rows, n_key), 0)
    own_head = (lane & 1) == ((row >> 3) & 1)
    late = (lane >> 1) - (row >> 4)
    out_lane = lax.broadcasted_iota(jnp.int32, (rows, lanes), 1)
    out_row = lax.broadcasted_iota(jnp.int32, (rows, lanes), 0)
    nothing = jnp.zeros((rows, n_key), BF16)

    @pl.loop(0, (n_used + 4 * quads - 1) // (4 * quads))
    def _(u):
        done = []
        for quad in range(quads):
            facts = []
            for t in range(4):
                i = (u * quads + quad) * 4 + t
                listed = info_ref[jnp.minimum(i, n_slots - 1)]
                used = (i < n_slots) & (listed >= 0)
                s = jnp.where(used, listed, 0)
                facts.append((s, used, jnp.maximum(info_ref[n_slots + s], 0), info_ref[2 * n_slots + s], info_ref[3 * n_slots + s]))
            q = jnp.concatenate([q_ref[f[2], :rows] for f in facts], axis=0)
            k = jnp.concatenate([kbuf[f[0]].reshape(n_key, lanes) for f in facts], axis=0)
            v = jnp.concatenate([vbuf[f[0]].reshape(n_key, lanes) for f in facts], axis=0)
            scores = lax.dot_general(q, k, (((1,), (1,)), ((), ())), preferred_element_type=F32)
            ps, stats = [], []
            for t, (s, used, b, lim, again) in enumerate(facts):
                sc = scores[t * rows:(t + 1) * rows, t * n_key:(t + 1) * n_key] * scale
                sc = jnp.where(own_head & (late <= lim), sc, NEG)
                m = jnp.max(sc, axis=1, keepdims=True)
                p = jnp.exp(sc - m)
                stats.append((m, jnp.sum(p, axis=1, keepdims=True)))
                ps.append(jnp.concatenate([p.astype(BF16) if x == t else nothing for x in range(4)], axis=1))
            o = jnp.dot(jnp.concatenate(ps, axis=0), v, preferred_element_type=F32)
            for t, (s, used, b, lim, again) in enumerate(facts):
                done.append((used, b, *stats[t], o[t * rows:(t + 1) * rows], again))
        for used, b0, m, l, o, again in done:
            def put(m, l, o):
                o_ref[b0] = o
                ml = jnp.where(out_lane == out_row, m, 0.0) + jnp.where(out_lane == out_row + rows, l, 0.0)
                ml_ref[pl.ds(b0, 1)] = jnp.sum(ml, axis=0, keepdims=True)

            @pl.when(used & (again == 0))
            def _():
                put(m, l, o)

            @pl.when(used & (again > 0))
            def _():
                old = jnp.broadcast_to(ml_ref[pl.ds(b0, 1)], (rows, lanes))
                m1 = jnp.sum(jnp.where(out_lane == out_row, old, 0.0), axis=1, keepdims=True)
                l1 = jnp.sum(jnp.where(out_lane == out_row + rows, old, 0.0), axis=1, keepdims=True)
                mm = jnp.maximum(m, m1)
                w, w1 = jnp.exp(m - mm), jnp.exp(m1 - mm)
                put(mm, l * w + l1 * w1, o * w + o_ref[b0] * w1)

    for c in outs:
        c.wait()


def mlp_kernel(layer, depth, more, attn_ref, hid_ref, wo_ref, up_ref, dn_ref, *rest):
    if more:
        wq_ref, wk_ref, wv_ref, out_ref, q_ref, k_ref, v_ref, abuf, bbuf, x_all, u, acc, got, a_sem, b_sem, send, recv, kvbuf, kv_sem = rest
        n_query = wq_ref.shape[2] // abuf.shape[2]
    else:
        out_ref, abuf, bbuf, x_all, u, acc, got, a_sem, b_sem, send, recv = rest
        n_query = 0
    kv = lax.axis_index('kv')
    core = kv % 2
    mate = kv + 1 - 2 * core
    width, tile = abuf.shape[1:]
    n_out = width // tile
    n_up = -(-up_ref.shape[2] // (2 * tile))
    base = core * (up_ref.shape[2] - n_up * tile)
    both = 2 * n_up * tile - up_ref.shape[2]
    chunk = 256

    def cols(t):
        return pl.ds(pl.multiple_of(base + t * tile, chunk), tile)

    def load_out(n):
        return pltpu.make_async_copy(wo_ref.at[layer, :, pl.ds(n * tile, tile)], abuf.at[n % depth], a_sem.at[n % depth])

    def load_up(t):
        slot = (t + n_out) % depth
        return pltpu.make_async_copy(up_ref.at[layer, :, cols(t)], abuf.at[slot], a_sem.at[slot])

    def load_query(j):
        slot = (j + n_out + n_up) % depth
        return pltpu.make_async_copy(wq_ref.at[layer + 1, :, pl.ds(pl.multiple_of(j * tile, tile), tile)], abuf.at[slot], a_sem.at[slot])

    def load_kv(i):
        return pltpu.make_async_copy((wk_ref, wv_ref)[i].at[layer + 1], kvbuf.at[i], kv_sem.at[i])

    def load_down(t):
        slot = t % depth
        return pltpu.make_async_copy(dn_ref.at[layer, cols(t), :], bbuf.at[slot], b_sem.at[slot])

    for n in range(min(depth, n_out)):
        load_out(n).start()
    for t in range(depth):
        load_down(t).start()
    barrier = pltpu.get_barrier_semaphore()
    pl.semaphore_signal(barrier, inc=1, device_id={'kv': mate}, device_id_type=MESH)
    pl.semaphore_wait(barrier, 1)

    def across(src, dst, i):
        return pltpu.make_async_remote_copy(
            src_ref=src, dst_ref=dst, send_sem=send.at[i], recv_sem=recv.at[i], device_id={'kv': mate}, device_id_type=MESH)

    for n in range(n_out):
        load_out(n).wait()
        part = slice(n * tile, (n + 1) * tile)
        y = jnp.dot(attn_ref[...], abuf[n % depth], preferred_element_type=F32)
        x_all[core, :, part] = (hid_ref[:, part].astype(F32) + y).astype(BF16)
        later = n + depth
        if later < n_out:
            load_out(later).start()
        else:
            load_up(later - n_out).start()
    if more:
        for i in range(2):
            load_kv(i).start()
    share = across(x_all.at[core], x_all.at[core], 0)
    share.start()
    acc[...] = jnp.zeros_like(acc)
    share.wait_send()
    across(x_all.at[core], x_all.at[1 - core], 0).wait_recv()

    @pl.loop(0, n_up)
    def _(t):
        slot = (t + n_out) % depth
        load_up(t).wait()
        x = x_all[...].reshape(-1, width)
        for c in range(tile // chunk):
            part = slice(c * chunk, (c + 1) * chunk)
            y = jax.nn.gelu(jnp.dot(x, abuf[slot, :, part], preferred_element_type=F32)).astype(BF16)
            if c * chunk < both:
                y = jnp.where((core == 1) & (t == 0), jnp.zeros_like(y), y)
            u[:, part] = y

        @pl.when(t + depth < n_up)
        def _():
            load_up(t + depth).start()

        if more:
            @pl.when((t + depth >= n_up) & (t + depth < n_up + n_query))
            def _():
                load_query(t + depth - n_up).start()

        load_down(t).wait()
        for c in range(width // tile):
            part = slice(c * tile, (c + 1) * tile)
            y = jnp.dot(u[...], bbuf[t % depth, :, part], preferred_element_type=F32)
            acc[:, :, part] += y.reshape(acc.shape[0], acc.shape[1], tile)

        @pl.when(t + depth < n_up)
        def _():
            load_down(t + depth).start()

    give = across(acc.at[1 - core], got, 1)
    give.start()
    give.wait()
    h = (x_all[core].astype(F32) + (acc[core] + got[...])).astype(BF16)
    out_ref[...] = h
    for j in range(n_query):
        load_query(j).wait()
        q_ref[:, j * tile:(j + 1) * tile] = jnp.dot(h, abuf[(j + n_out + n_up) % depth], preferred_element_type=F32).astype(BF16)
    if more:
        for i, o in enumerate((k_ref, v_ref)):
            load_kv(i).wait()
            o[...] = jnp.dot(h, kvbuf[i], preferred_element_type=F32).astype(BF16)


def blank_kernel(o_ref):
    pass


def sems(*shape):
    return pltpu.SemaphoreType.DMA(shape)


def comm(cid, mib=None):
    return pltpu.CompilerParams(collective_id=cid, has_side_effects=True, **({'vmem_limit_bytes': mib << 20} if mib else {}))


def solution(mesh):
    n_rows = mesh.shape['kv2']
    n_cols = mesh.shape['kv']
    n_dev = n_rows * n_cols
    dev_axes = ('rep', 'kv2', 'kv')
    seq_spec = P(None, dev_axes, None)
    pool_spec = P(dev_axes, None, None, None, None)
    table_spec = P(dev_axes, None)
    vec_spec = P(dev_axes)
    full_spec = P()

    def per_device(x_embed, w_query, w_key, w_value, w_out, w_up, w_down, k_pool, v_pool, old_table, seq_len, src_slot, dst_slot):
        n_slots, layers, page, kv_heads, head_dim = k_pool.shape
        heads = w_query.shape[2] // head_dim
        n_steps, seq_dev, width = x_embed.shape
        n_moves = src_slot.shape[0]
        row_seqs = seq_dev * n_cols
        rows = n_steps * heads
        key_rows = page * kv_heads
        tile = 8
        n_ch = key_rows // tile
        chunks = 2 * n_ch
        cap = 20
        assert chunks == n_dev and rows == 32 and old_table.shape[1] == 2
        shift = 18
        magic = -(-(1 << shift) // n_slots)
        assert all((s * magic) >> shift == s // n_slots for s in range(n_dev * n_slots))
        me = flat_id(n_cols)
        who = jnp.stack([me, lax.axis_index('kv2') * n_cols, lax.axis_index('kv') % 2]).astype(jnp.int32)

        kp = k_pool.reshape(n_slots, layers, n_ch, tile, head_dim)
        vp = v_pool.reshape(n_slots, layers, n_ch, tile, head_dim)
        kp4 = k_pool.reshape(n_slots, layers * n_ch, tile, head_dim)
        vp4 = v_pool.reshape(n_slots, layers * n_ch, tile, head_dim)
        packed = pl.pallas_call(
            functools.partial(pack_kernel, n_moves),
            out_shape=[jax.ShapeDtypeStruct((chunks, n_moves, tile, head_dim), BF16)] * layers,
            in_specs=[SMEM, ANY, ANY], out_specs=[VMEM] * layers,
            scratch_shapes=[sems(layers, 2, n_moves)], name='pack_pages')(src_slot - me * n_slots, kp, vp)
        after = lax.optimization_barrier

        mine = jnp.concatenate([old_table.reshape(-1), seq_len, src_slot, dst_slot])
        mine = jnp.pad(mine, (0, 128 - mine.shape[0])).reshape(1, 128)
        tab = pl.pallas_call(
            functools.partial(gather_all_kernel, n_dev, n_cols),
            out_shape=jax.ShapeDtypeStruct((n_dev, 1, 128), jnp.int32),
            in_specs=[VMEM], out_specs=VMEM,
            scratch_shapes=[pltpu.SemaphoreType.DMA, sems(n_dev), sems(n_dev)],
            compiler_params=comm(0), name='gather_tables')(mine)

        tab = tab.reshape(n_dev, 128)
        moving, tab = after((packed[0], tab))
        spread = lax.all_to_all(moving, ('kv2', 'kv'), 0, 0, tiled=True)
        dims = (n_dev, n_cols, n_slots, seq_dev, n_moves, cap, page, magic, shift)
        pages, arrive, most = pl.pallas_call(
            functools.partial(places_kernel, dims),
            out_shape=(jax.ShapeDtypeStruct((n_dev * cap + 1,), jnp.int32), jax.ShapeDtypeStruct((3 * n_slots + 1,), jnp.int32),
                       jax.ShapeDtypeStruct((2,), jnp.int32)),
            in_specs=[SMEM, SMEM], out_specs=(SMEM, SMEM, SMEM),
            scratch_shapes=[pltpu.SMEM((n_dev // 2,), jnp.int32)], name='places')(who, tab)

        def regroup(spread, name):
            return pl.pallas_call(
                functools.partial(regroup_kernel, cap),
                out_shape=jax.ShapeDtypeStruct((n_dev, cap, tile, head_dim), BF16),
                in_specs=[SMEM, VMEM], out_specs=VMEM, compiler_params=pltpu.CompilerParams(vmem_limit_bytes=46 << 20), name=name)(pages, spread.reshape(n_dev * n_moves, tile, head_dim))

        def deliver(grouped):
            return lax.all_to_all(grouped, ('kv2', 'kv'), 0, 0, tiled=True)

        def to_mate(own):
            return lax.ppermute(own, 'kv', [(i, i ^ 1) for i in range(n_cols)])

        def all_pages():
            found = []
            for p in packed:
                everything = lax.all_gather(p.swapaxes(0, 1), ('kv2', 'kv'), tiled=True)
                found.append(everything[jnp.maximum(arrive[n_slots:2 * n_slots], 0)])
            return jnp.stack(found)

        def no_pages():
            return pl.pallas_call(
                blank_kernel, out_shape=jax.ShapeDtypeStruct((layers, n_slots, chunks, tile, head_dim), BF16), out_specs=ANY,
                name='blank')()

        slow = lax.cond(most[0] > 2 * cap, all_pages, no_pages)

        hidden = x_embed.reshape(n_steps * seq_dev, width)
        k_out = v_out = None
        for layer in range(layers):
            if layer == 0:
                query, k_new, v_new = (jnp.dot(hidden, w[layer], preferred_element_type=F32).astype(BF16) for w in (w_query, w_key, w_value))

            def by_seq(x):
                return x.reshape(n_steps, seq_dev, -1, head_dim).swapaxes(0, 1).reshape(seq_dev, -1, head_dim)

            load = jnp.concatenate([by_seq(query), by_seq(k_new), by_seq(v_new)], axis=1)
            q_rows = load.shape[1]
            if layer == 0:
                spread, load, pages = after((spread, load, pages))
                grouped, load, tab = after((regroup(spread, 'regroup_pages_0'), load, tab))
                own = deliver(grouped)
                info, n_used = pl.pallas_call(
                    functools.partial(cells_kernel, dims),
                    out_shape=(jax.ShapeDtypeStruct((4 * n_slots + 1,), jnp.int32), jax.ShapeDtypeStruct((1,), jnp.int32)),
                    in_specs=[SMEM, SMEM, ANY], out_specs=(SMEM, SMEM),
                    scratch_shapes=[pltpu.SMEM((n_dev * n_slots,), jnp.int32), pltpu.SMEM((row_seqs + 1,), jnp.int32), pltpu.SemaphoreType.DMA],
                    name='cells')(who, tab, jnp.full((n_dev * n_slots,), -1, jnp.int32))
                pool_shape = jax.ShapeDtypeStruct(kp4.shape, BF16)
                load, info = after((load, info))
            else:
                own, load = after((own, load))
                mate = to_mate(own)
            n_chips = n_cols // 2
            q_row = pl.pallas_call(
                functools.partial(row_gather_kernel, n_cols),
                out_shape=jax.ShapeDtypeStruct((n_cols, seq_dev, q_rows, head_dim), BF16),
                in_specs=[VMEM], out_specs=VMEM,
                scratch_shapes=[pltpu.SemaphoreType.DMA, sems(n_chips), sems(n_chips), sems(n_chips), sems(n_chips)],
                compiler_params=comm(3 + layer, 40), name=f'gather_queries_{layer}')(load)

            first = layer == 0
            if first:
                own, q_row = after((own, q_row))
                mate = to_mate(own)
            last = layer == layers - 1
            if not last:
                moving, q_row = after((packed[layer + 1], q_row))
                spread = lax.all_to_all(moving, ('kv2', 'kv'), 0, 0, tiled=True)
            carried = () if first else (k_out, v_out)
            k_out, v_out, part, ml = pl.pallas_call(
                functools.partial(attend_kernel, (layer, n_slots, cap, head_dim ** -0.5, 2, first)),
                in_specs=[SMEM] * 5 + [VMEM] + [ANY] * (5 + len(carried)),
                out_specs=[ANY, ANY, VMEM, VMEM],
                out_shape=[pool_shape, pool_shape, jax.ShapeDtypeStruct((row_seqs, rows, head_dim), F32),
                           jax.ShapeDtypeStruct((row_seqs, head_dim), F32)],
                scratch_shapes=[pltpu.VMEM((n_slots, n_ch, tile, head_dim), BF16), pltpu.VMEM((n_slots, n_ch, tile, head_dim), BF16),
                                sems(2), sems(2), sems(2, n_slots)],
                input_output_aliases={} if first else {11: 0, 12: 1},
                compiler_params=pltpu.CompilerParams(vmem_limit_bytes=46 << 20), name=f'attend_{layer}')(who, arrive, most, info, n_used, q_row.reshape(row_seqs, q_rows, head_dim), kp4, vp4,
                                        own, mate, slow, *carried)

            parts, parts_ml = (n_chips, seq_dev, rows, head_dim), (n_chips, seq_dev, head_dim)
            attn = pl.pallas_call(
                functools.partial(return_kernel, n_cols),
                out_shape=jax.ShapeDtypeStruct((n_steps, seq_dev, heads, head_dim), BF16),
                in_specs=[VMEM, VMEM], out_specs=VMEM,
                scratch_shapes=[pltpu.VMEM(shape, F32) for _ in range(3) for shape in (parts, parts_ml)] + [sems(2, n_chips)] * 4,
                compiler_params=comm(5 + layer, 40), name=f'return_{layer}')(
                    part.reshape(n_cols, seq_dev, rows, head_dim), ml.reshape(n_cols, seq_dev, head_dim))
            attn_out = attn.reshape(n_steps * seq_dev, heads * head_dim)
            n_tok = n_steps * seq_dev
            if not last:
                spread, attn_out = after((spread, attn_out))
                grouped, attn_out = after((regroup(spread, f'regroup_pages_{layer + 1}'), attn_out))
                own = deliver(grouped)
            depth, wide = 4, 512
            assert w_up.shape[2] % 256 == 0 and width % wide == 0
            kv_width = w_key.shape[2]
            extra = () if last else (w_query, w_key, w_value)
            assert w_query.shape[2] // wide == depth
            hidden, *proj = pl.pallas_call(
                functools.partial(mlp_kernel, layer, depth, not last),
                out_shape=[jax.ShapeDtypeStruct((n_tok, n), BF16)
                           for n in ((width,) if last else (width, w_query.shape[2], kv_width, kv_width))],
                in_specs=[VMEM, VMEM, ANY, ANY, ANY] + [ANY] * len(extra), out_specs=[VMEM] * (1 if last else 4),
                scratch_shapes=[pltpu.VMEM((depth, width, wide), BF16), pltpu.VMEM((depth, wide, width), BF16),
                                pltpu.VMEM((2, n_tok, width), BF16), pltpu.VMEM((2 * n_tok, wide), BF16),
                                pltpu.VMEM((2, n_tok, width), F32), pltpu.VMEM((n_tok, width), F32),
                                sems(depth), sems(depth), sems(2), sems(2)]
                               + ([] if last else [pltpu.VMEM((2, width, kv_width), BF16), sems(2)]),
                compiler_params=comm(7 + layer, 52), name=f'mlp_{layer}')(attn_out, hidden, w_out, w_up, w_down, *extra)
            if not last:
                query, k_new, v_new = proj
        return hidden.reshape(x_embed.shape), k_out.reshape(k_pool.shape), v_out.reshape(v_pool.shape)

    return jax.shard_map(per_device, mesh=mesh, in_specs=(seq_spec, full_spec, full_spec, full_spec, full_spec, full_spec, full_spec, pool_spec, pool_spec, table_spec, vec_spec, vec_spec, vec_spec), out_specs=(seq_spec, pool_spec, pool_spec), check_vma=False)
```
